256 devices in a mesh: space: 32 (over y, z_hi, core), filt: 8 (over z_lo, x).
Axes of the slice: x: 4, y: 4, z: 8 (z_hi: 4, z_lo: 2; z = z_hi * 2 + z_lo), core: 2. Of those that a mesh axis runs over, the one named last changes fastest.
Arguments:
- volume: bfloat16 [64, 64, 16, 256], P(None, 'space', 'filt'), may hold values from -6 to 6
- first_weight: bfloat16 [27, 64, 64], replicated, may hold values from -0.15625 to 0.15625
- second_weight: bfloat16 [27, 128, 64], P(None, 'filt'), may hold values from -0.15625 to 0.15625
- cotangent: bfloat16 [128, 32, 8, 128], P('filt', 'space'), may hold values from -24 to 24
Outputs:
- features: bfloat16 [128, 32, 8, 128], P('filt', 'space')
- volume_grad: bfloat16 [64, 64, 16, 256], P(None, 'space', 'filt')
- first_grad: float32 [27, 64, 64], replicated
- second_grad: float32 [27, 128, 64], P(None, 'filt')
The draws below stay inside these ranges and needn't reach their ends.
All inputs are finite; a program needn't handle non-finite values.
Results may differ from the reference program's by a relative error of at most 0.019.
Values may be sent and summed in bfloat16 or wider, within the bound.
A program may use at most 64 MiB of HBM per device.

```python
import jax
import jax.numpy as jnp
from jax import lax

C1 = 64
C2 = 128
Z3 = 128
X3 = 32
Y3 = 8
X2 = 64
Y2 = 16
Z2 = 256
N_FILT = 8


def shard_levels(own_key, dims, cuts, smallest, largest):
    def one(position, shards_of):
        heights = jax.random.uniform(jax.random.fold_in(jax.random.fold_in(own_key, 6), position), (shards_of,), jnp.float32, smallest / len(cuts), largest / len(cuts))
        return jnp.repeat(jnp.exp(heights), dims[position] // shards_of).reshape((-1,) + (1,) * (len(dims) - position - 1))

    factor_of = one(*cuts[0])
    for cut in cuts[1:]:
        factor_of = factor_of * one(*cut)
    return factor_of


def noise(stream_key, dims, scale, most, shards=(), dtype=jnp.bfloat16):
    values = scale * jax.random.normal(stream_key, dims, jnp.float32)
    if shards:
        values = values * shard_levels(stream_key, dims, shards, -0.22, 0.18)
    return jnp.clip(values, -most, most).astype(dtype)


def setup_inputs(seed: int = 0) -> dict:
    splits = jax.random.split(jax.random.key(seed), 5)
    return {
        "volume": noise(splits[0], (C1, X2, Y2, Z2), 1.0, 6.0, ((1, 32), (2, 8))),
        "first_weight": noise(splits[1], (27, C1, C1), (27 * C1) ** -0.5, 0.15625),
        "second_weight": noise(splits[2], (27, C2, C1), (27 * C1) ** -0.5, 0.15625, ((1, 8),)),
        "cotangent": noise(splits[3], (C2, X3, Y3, Z3), 4.0, 24.0, ((0, 8), (1, 32))),
    }


def silu_slope(values):
    sigmoid_part = jax.nn.sigmoid(values)
    return sigmoid_part * (1.0 + values * (1.0 - sigmoid_part))


def pad_all(volume_field):
    return jnp.pad(volume_field, ((0, 0), (1, 1), (1, 1), (1, 1)))


def window(padded, offset_x, offset_y, offset_z, extents):
    extent_x, extent_y, extent_z = extents
    section = lax.slice(padded, (0, offset_x, offset_y, offset_z), (padded.shape[0], offset_x + extent_x, offset_y + extent_y, offset_z + extent_z))
    return section.reshape(padded.shape[0], extent_x * extent_y * extent_z)


def conv_forward(padded, weight, extents):
    outputs, inputs = weight.shape[1], weight.shape[2]
    running = jnp.zeros((outputs, extents[0] * extents[1] * extents[2]), jnp.float32)
    for offset_x in range(3):
        for offset_y in range(3):
            tap_base = offset_x * 9 + offset_y * 3
            stacked = jnp.concatenate([window(padded, offset_x, offset_y, offset_z, extents) for offset_z in range(3)], axis=0)
            matrices = jnp.transpose(weight[tap_base:tap_base + 3], (1, 0, 2)).reshape(outputs, 3 * inputs)
            running = running + jnp.dot(matrices, stacked, preferred_element_type=jnp.float32)
    return running


def conv_transpose(padded, weight, extents):
    outputs, inputs = weight.shape[1], weight.shape[2]
    running = jnp.zeros((inputs, extents[0] * extents[1] * extents[2]), jnp.float32)
    for offset_x in range(3):
        for offset_y in range(3):
            tap_base = offset_x * 9 + offset_y * 3
            stacked = jnp.concatenate([window(padded, offset_x, offset_y, offset_z, extents) for offset_z in range(3)], axis=0)
            tap_block = weight[24 - tap_base:27 - tap_base][::-1]
            matrices = jnp.transpose(tap_block, (2, 0, 1)).reshape(inputs, 3 * outputs)
            running = running + jnp.dot(matrices, stacked, preferred_element_type=jnp.float32)
    return running


def conv_weights(grad_rows, padded, extents):
    outputs, inputs = grad_rows.shape[0], padded.shape[0]
    blocks = []
    for offset_x in range(3):
        for offset_y in range(3):
            stacked = jnp.concatenate([window(padded, offset_x, offset_y, offset_z, extents) for offset_z in range(3)], axis=0)
            section = lax.dot_general(grad_rows, stacked, (((1,), (1,)), ((), ())), preferred_element_type=jnp.float32)
            blocks.append(jnp.transpose(section.reshape(outputs, 3, inputs), (1, 0, 2)))
    return jnp.concatenate(blocks, axis=0)


def pool_cells(hidden):
    channels, size_x, size_y, size_z = hidden.shape
    pair_table = (jnp.arange(size_z)[:, None] // 2 == jnp.arange(size_z // 2)[None, :]).astype(jnp.bfloat16)
    depth_sums = jnp.dot(hidden.reshape(-1, size_z), pair_table, preferred_element_type=jnp.float32)
    depth_sums = depth_sums.reshape(channels, size_x // 2, 2, size_y // 2, 2, size_z // 2)
    return (0.125 * depth_sums.sum(axis=(2, 4))).astype(jnp.bfloat16)


def spread_cells(grad_field):
    scaled = 0.125 * grad_field
    scaled = jnp.repeat(scaled, 2, axis=1)
    scaled = jnp.repeat(scaled, 2, axis=2)
    return jnp.repeat(scaled, 2, axis=3)


def reference(volume, first_weight, second_weight, cotangent):
    channels = volume.shape[0]
    fine_shape = volume.shape[1:]
    padded_in = pad_all(volume)
    first_pre = conv_forward(padded_in, first_weight, fine_shape)
    hidden = jax.nn.silu(first_pre).astype(jnp.bfloat16).reshape((channels,) + fine_shape)
    pooled = pool_cells(hidden)
    slab_shape = pooled.shape[1:]
    padded_pool = pad_all(pooled)
    second_pre = conv_forward(padded_pool, second_weight, slab_shape)
    total_filters = second_weight.shape[1]
    features = jax.nn.silu(second_pre).astype(jnp.bfloat16).reshape((total_filters,) + slab_shape)
    down_grad = (cotangent.reshape(total_filters, -1).astype(jnp.float32) * silu_slope(second_pre)).astype(jnp.bfloat16)
    bottom_scale = 1.0 / (slab_shape[0] * slab_shape[1] * slab_shape[2]) ** 0.5
    second_grad = conv_weights(down_grad, padded_pool, slab_shape) * bottom_scale
    padded_down = pad_all(down_grad.reshape((total_filters,) + slab_shape))
    group_size = total_filters // N_FILT
    pool_grad = jnp.zeros((channels, slab_shape[0] * slab_shape[1] * slab_shape[2]), jnp.float32)
    for group_index in range(N_FILT):
        lower = group_index * group_size
        section = conv_transpose(padded_down[lower:lower + group_size], second_weight[:, lower:lower + group_size], slab_shape)
        pool_grad = pool_grad + lax.optimization_barrier(section.astype(jnp.bfloat16)).astype(jnp.float32)
    hidden_grad = spread_cells(pool_grad.reshape((channels,) + slab_shape))
    first_down = (hidden_grad.reshape(channels, -1) * silu_slope(first_pre)).astype(jnp.bfloat16)
    fine_scale = 1.0 / (fine_shape[0] * fine_shape[1] * fine_shape[2]) ** 0.5
    first_grad = conv_weights(first_down, padded_in, fine_shape) * fine_scale
    padded_back = pad_all(first_down.reshape((channels,) + fine_shape))
    volume_grad = conv_transpose(padded_back, first_weight, fine_shape).astype(jnp.bfloat16).reshape((channels,) + fine_shape)
    return (features, volume_grad, first_grad, second_grad)
```

```python
import functools

import jax
import jax.numpy as jnp
from jax import lax
from jax.experimental import pallas as pl
from jax.experimental.pallas import tpu as pltpu
from jax.sharding import PartitionSpec as P

MESH = pl.DeviceIdType.MESH
F32 = jnp.float32
BF16 = jnp.bfloat16
DIRS = [(dx, dy) for dx in (-1, 0, 1) for dy in (-1, 0, 1) if (dx, dy) != (0, 0)]
N_SEMS = 128


def sigmoid(v):
    return 1.0 / (1.0 + jnp.exp(-v))


def shifted(values, by):
    if by == 0:
        return values
    length = values.shape[1]
    lane = lax.broadcasted_iota(jnp.int32, values.shape, 1)
    if by == 1:
        return jnp.where(lane == length - 1, 0.0, pltpu.roll(values, length - 1, 1))
    return jnp.where(lane == 0, 0.0, pltpu.roll(values, 1, 1))


def nt_dot(a, b):
    return lax.dot_general(a, b, (((1,), (1,)), ((), ())), preferred_element_type=F32)


def kernel(
    sizes,
    vol,
    cot,
    w1f,
    w1b,
    w2l,
    feat_out,
    vgrad_out,
    g1_out,
    g2_out,
    ext,
    fd,
    extd,
    slope1,
    cotg,
    w2g,
    w2b,
    ps,
    ds,
    featb,
    s_gb,
    s_cb,
    s_pb,
    s_fb,
    s_yr,
    s_zr,
    s_os,
    f_gb,
    f_cb,
    f_pb,
    f_fb,
    f_yr,
    f_zr,
    f_ag,
    send_sem,
    recv_sem,
):
    n_s, n_f, n_y, n_z = sizes
    s = lax.axis_index("space")
    f = lax.axis_index("filt")
    core = lax.rem(s, 2)
    zh = lax.rem(s // 2, n_z)
    y = s // (2 * n_z)
    fine_scale = 1.0 / float(n_s * 2 * n_f * 2 * 256) ** 0.5
    bottom_scale = 1.0 / float(n_s * n_f * 128) ** 0.5

    def near(dx, dy):
        return (lax.rem(s + dx + n_s, n_s), lax.rem(f + dy + n_f, n_f))

    def along_f(j):
        return (s, lax.rem(f + j, n_f))

    def along_y(j):
        return ((lax.rem(y + j, n_y) * n_z + zh) * 2 + core, f)

    def along_z(j):
        return ((y * n_z + lax.rem(zh + j, n_z)) * 2 + core, f)

    twin = (s + 1 - 2 * core, f)

    peers = [near(dx, dy) for dx, dy in DIRS]
    peers += [along_f(j) for j in range(1, n_f)]
    peers += [along_y(j) for j in range(1, n_y)]
    peers += [along_z(j) for j in range(1, n_z)]
    peers += [twin]
    barrier = pltpu.get_barrier_semaphore()
    for peer in peers:
        pl.semaphore_signal(barrier, inc=1, device_id=peer, device_id_type=MESH)
    pl.semaphore_wait(barrier, len(peers))

    sent = []

    def send(src, dst, device):
        at = len(sent)
        copy = pltpu.make_async_remote_copy(
            src_ref=src,
            dst_ref=dst,
            send_sem=send_sem.at[at],
            recv_sem=recv_sem.at[at],
            device_id=device,
            device_id_type=MESH,
        )
        copy.start()
        sent.append(copy)
        return at

    def arrive(ref, at):
        pltpu.make_async_copy(ref, ref, recv_sem.at[at]).wait()

    def src_part(d):
        return {1: 1, -1: 0, 0: slice(None)}[d]

    def dst_part(d):
        return {1: 0, -1: 3, 0: slice(1, 3)}[d]

    def halo_start(brick, field):
        out = []
        for dx, dy in DIRS:
            target = field.at[dst_part(dx), dst_part(dy)]
            out.append((send(brick.at[src_part(dx), src_part(dy)], target, near(dx, dy)), target))
        return out

    def finish(waits):
        for at, ref in waits:
            arrive(ref, at)

    def zero_rim(field, last):
        @pl.when(s == 0)
        def _():
            for b in range(last + 1):
                field[0, b] = jnp.zeros(field.shape[2:], field.dtype)

        @pl.when(s == n_s - 1)
        def _():
            for b in range(last + 1):
                field[last, b] = jnp.zeros(field.shape[2:], field.dtype)

        @pl.when(f == 0)
        def _():
            for a in range(last + 1):
                field[a, 0] = jnp.zeros(field.shape[2:], field.dtype)

        @pl.when(f == n_f - 1)
        def _():
            for a in range(last + 1):
                field[a, last] = jnp.zeros(field.shape[2:], field.dtype)

    vol_waits = halo_start(vol, ext)
    cot_waits = []
    w2_waits = []
    for j in range(1, n_f):
        other = lax.rem(f + j, n_f)
        source = lax.rem(f - j + n_f, n_f)
        cot_waits.append((send(cot.at[other], cotg.at[f], along_f(j)), cotg.at[source]))
    for j in range(1, n_f):
        source = lax.rem(f - j + n_f, n_f)
        w2_waits.append((send(w2l, w2g.at[f], along_f(j)), w2g.at[source]))
    for a in range(2):
        for b in range(2):
            ext[a + 1, b + 1] = vol[a, b]
    cotg[f] = cot[f]
    w2g[f] = w2l[...]
    ps[3, 0] = jnp.zeros((64, 128), BF16)
    pair_row = lax.broadcasted_iota(jnp.int32, (256, 128), 0)
    pair_col = lax.broadcasted_iota(jnp.int32, (256, 128), 1)
    below = pair_row - 2 * pair_col
    pairs = jnp.where((below == 0) | (below == 1), 1.0, 0.0).astype(BF16)

    def stack(field, a, b):
        planes = [field[a + i, b + j] for i in range(3) for j in range(3)]
        return jnp.concatenate(planes + [jnp.zeros((64, 256), BF16)], axis=0)

    finish(vol_waits)
    zero_rim(ext, 3)

    wf = w1f[...]
    total = jnp.zeros((64, 128), F32)
    for a in range(2):
        for b in range(2):
            rows = jnp.dot(wf, stack(ext, a, b), preferred_element_type=F32)
            pre = shifted(rows[0:64], -1) + rows[64:128] + shifted(rows[128:192], 1)
            gate = sigmoid(pre)
            slope1[a, b] = gate * (1.0 + pre * (1.0 - gate))
            hidden = (pre * gate).astype(BF16)
            total = total + jnp.dot(hidden, pairs, preferred_element_type=F32)
    ps[1, 1] = (0.125 * total).astype(BF16)

    pool_waits = []
    for dx, dy in DIRS:
        target = ps.at[1 - dx, 1 - dy]
        pool_waits.append((send(ps.at[1, 1], target, near(dx, dy)), target))

    finish(cot_waits)
    finish(w2_waits)
    w2 = w2g[...].reshape(n_f * 48, 640)
    for dz in range(3):
        block = w2g[:, 16 * dz : 16 * dz + 16, :].reshape(128, 640).astype(F32)
        turned = block.T.astype(BF16)
        for slot in range(9):
            w2b[64 * dz : 64 * dz + 64, 128 * (8 - slot) : 128 * (8 - slot) + 128] = turned[
                64 * slot : 64 * slot + 64
            ]

    finish(pool_waits)
    zero_rim(ps, 2)

    around = jnp.concatenate(
        [ps[i, j] for i in range(3) for j in range(3)] + [ps[3, 0]], axis=0
    )
    rows = jnp.dot(w2, around, preferred_element_type=F32).reshape(n_f, 3, 16, 128)
    pre = (
        shifted(rows[:, 0].reshape(128, 128), -1)
        + rows[:, 1].reshape(128, 128)
        + shifted(rows[:, 2].reshape(128, 128), 1)
    )
    gate = sigmoid(pre)
    down = cotg[...].reshape(128, 128).astype(F32) * (gate * (1.0 + pre * (1.0 - gate)))
    ds[1, 1] = down.astype(BF16)
    featb[0] = (pre * gate).astype(BF16).reshape(n_f, 16, 128)

    down_waits = []
    for dx, dy in DIRS:
        target = ds.at[1 - dx, 1 - dy]
        down_waits.append((send(ds.at[1, 1], target, near(dx, dy)), target))
    feat_waits = []
    for j in range(1, n_f):
        other = lax.rem(f + j, n_f)
        source = lax.rem(f - j + n_f, n_f)
        feat_waits.append(
            (send(featb.at[0, other], featb.at[1, f], along_f(j)), featb.at[1, source])
        )
    featb[1, f] = featb[0, f]

    moved = [shifted(down, 1).astype(BF16), down.astype(BF16), shifted(down, -1).astype(BF16)]
    lhs = jnp.concatenate(
        [moved[dz][16 * g : 16 * g + 16] for g in range(n_f) for dz in range(3)], axis=0
    )
    terms = nt_dot(lhs, around)

    def deal(values, height, buffer):
        per = values.shape[0] // n_f
        for g in range(n_f):
            tiles = [
                values[per * g + height * r : per * g + height * r + height, 128 * c : 128 * c + 128]
                for r in range(3)
                for c in range(5)
            ]
            tiles.append(jnp.zeros((height, 128), F32))
            for half in range(2):
                piece = jnp.concatenate(tiles[8 * half : 8 * half + 8], axis=0)
                buffer[half, g] = piece.astype(BF16)

    deal(terms, 16, s_gb)

    def to_twin(gb, cb):
        return [(send(gb.at[1 - core], cb, twin), cb)]

    def over_filt(gb, cb, pb, fb):
        pb[...] = (gb[core].astype(F32) + cb[...].astype(F32)).astype(BF16)
        fb[f] = pb[f]
        waits = []
        for j in range(1, n_f):
            other = lax.rem(f + j, n_f)
            source = lax.rem(f - j + n_f, n_f)
            waits.append((send(pb.at[other], fb.at[f], along_f(j)), fb.at[source]))
        return waits

    def summed(ref, count):
        value = ref[0].astype(F32)
        for k in range(1, count):
            value = value + ref[k].astype(F32)
        return value.astype(BF16)

    def over_y(fb, yr):
        yr[y] = summed(fb, n_f)
        waits = []
        for j in range(1, n_y):
            source = lax.rem(y - j + n_y, n_y)
            waits.append((send(yr.at[y], yr.at[y], along_y(j)), yr.at[source]))
        return waits

    def over_z(yr, zr):
        zr[zh] = summed(yr, n_y)
        waits = []
        for j in range(1, n_z):
            source = lax.rem(zh - j + n_z, n_z)
            waits.append((send(zr.at[zh], zr.at[zh], along_z(j)), zr.at[source]))
        return waits

    s_waits = to_twin(s_gb, s_cb)

    finish(down_waits)
    zero_rim(ds, 2)
    planes = jnp.concatenate([ds[i, j] for i in range(3) for j in range(3)], axis=0)
    rows = jnp.dot(w2b[...], planes, preferred_element_type=F32)
    pool_grad = 0.125 * (
        shifted(rows[0:64], 1) + rows[64:128] + shifted(rows[128:192], -1)
    )
    high = pool_grad.astype(BF16)
    low = (pool_grad - high.astype(F32)).astype(BF16)
    spread = nt_dot(jnp.concatenate([high, low], axis=0), pairs)
    spread = spread[0:64] + spread[64:128]
    for a in range(2):
        for b in range(2):
            fd[a, b] = (spread * slope1[a, b]).astype(BF16)
    fd_waits = halo_start(fd, extd)

    terms = jnp.zeros((192, 640), F32)
    for a in range(2):
        for b in range(2):
            own = fd[a, b]
            extd[a + 1, b + 1] = own
            wide = own.astype(F32)
            lhs = jnp.concatenate(
                [shifted(wide, 1).astype(BF16), own, shifted(wide, -1).astype(BF16)], axis=0
            )
            terms = terms + nt_dot(lhs, stack(ext, a, b))
    deal(terms, 8, f_gb)
    f_waits = to_twin(f_gb, f_cb)

    finish(s_waits)
    s_waits = over_filt(s_gb, s_cb, s_pb, s_fb)
    finish(f_waits)
    f_waits = over_filt(f_gb, f_cb, f_pb, f_fb)

    finish(fd_waits)
    zero_rim(extd, 3)
    wb = w1b[...]
    for a in range(2):
        for b in range(2):
            rows = jnp.dot(wb, stack(extd, a, b), preferred_element_type=F32)
            vgrad_out[a, b] = (
                shifted(rows[0:64], 1) + rows[64:128] + shifted(rows[128:192], -1)
            ).astype(BF16)
    finish(feat_waits)
    feat_out[...] = featb[1]

    finish(f_waits)
    f_waits = over_y(f_fb, f_yr)
    finish(s_waits)
    s_waits = over_y(s_fb, s_yr)
    finish(f_waits)
    f_waits = over_z(f_yr, f_zr)
    finish(s_waits)
    s_waits = over_z(s_yr, s_zr)
    finish(f_waits)
    f_ag[core, f] = summed(f_zr, n_z)
    f_waits = []
    for j in range(1, n_f):
        source = lax.rem(f - j + n_f, n_f)
        f_waits.append((send(f_ag.at[core, f], f_ag.at[core, f], along_f(j)), f_ag.at[core, source]))
    finish(s_waits)
    s_os[core] = summed(s_zr, n_z)
    s_waits = [(send(s_os.at[core], s_os.at[core], twin), s_os.at[1 - core])]
    finish(s_waits)

    def lay_out(read, height, scale, store):
        for k in range(15):
            tile = read(k) * scale
            dz, c = k // 5, k % 5
            store(6 * c + dz, tile[:, 0:64])
            if c < 4:
                store(6 * c + 3 + dz, pltpu.roll(tile, 64, 1)[:, 0:64])

    halves = [s_os[h].astype(F32) for h in range(2)]

    def store_bottom(tap, value):
        g2_out[tap] = value

    lay_out(
        lambda k: halves[k // 8][16 * (k % 8) : 16 * (k % 8) + 16], 16, bottom_scale, store_bottom
    )

    finish(f_waits)
    f_waits = [(send(f_ag.at[core], f_ag.at[core], twin), f_ag.at[1 - core])]
    finish(f_waits)
    for g in range(n_f):
        both = [f_ag[h, g].astype(F32) for h in range(2)]
        for k in range(15):
            row = 24 * g + 8 * (k // 5)
            dz, o = row // 64, row % 64
            c = k % 5
            tile = both[k // 8][8 * (k % 8) : 8 * (k % 8) + 8] * fine_scale
            g1_out[6 * c + dz, o : o + 8] = tile[:, 0:64]
            if c < 4:
                g1_out[6 * c + 3 + dz, o : o + 8] = pltpu.roll(tile, 64, 1)[:, 0:64]

    for copy in sent:
        copy.wait_send()


def local(sizes, volume, first_weight, second_weight, cotangent):
    n_s, n_f, n_y, n_z = sizes
    vol = jnp.transpose(volume, (1, 2, 0, 3))
    cot = jnp.transpose(cotangent[:, 0], (1, 0, 2))
    pad = ((0, 0), (0, 64))
    taps = first_weight.reshape(9, 3, 64, 64)
    w1f = jnp.pad(jnp.transpose(taps, (1, 2, 0, 3)).reshape(192, 576), pad)
    w1b = jnp.pad(jnp.transpose(taps[::-1], (1, 3, 0, 2)).reshape(192, 576), pad)
    bottom = second_weight.reshape(9, 3, 16, 64)
    w2l = jnp.pad(jnp.transpose(bottom, (1, 2, 0, 3)).reshape(48, 576), pad)
    vmem = pl.BlockSpec(memory_space=pltpu.VMEM)
    features, volume_grad, first_grad, second_grad = pl.pallas_call(
        functools.partial(kernel, sizes),
        out_shape=(
            jax.ShapeDtypeStruct((n_f, 16, 128), BF16),
            jax.ShapeDtypeStruct((2, 2, 64, 256), BF16),
            jax.ShapeDtypeStruct((27, 64, 64), F32),
            jax.ShapeDtypeStruct((27, 16, 64), F32),
        ),
        in_specs=[vmem] * 5,
        out_specs=(vmem,) * 4,
        scratch_shapes=[
            pltpu.VMEM((4, 4, 64, 256), BF16),
            pltpu.VMEM((2, 2, 64, 256), BF16),
            pltpu.VMEM((4, 4, 64, 256), BF16),
            pltpu.VMEM((2, 2, 64, 256), F32),
            pltpu.VMEM((n_f, 16, 128), BF16),
            pltpu.VMEM((n_f, 48, 640), BF16),
            pltpu.VMEM((192, 1152), BF16),
            pltpu.VMEM((4, 3, 64, 128), BF16),
            pltpu.VMEM((3, 3, 128, 128), BF16),
            pltpu.VMEM((2, n_f, 16, 128), BF16),
            pltpu.VMEM((2, n_f, 128, 128), BF16),
            pltpu.VMEM((n_f, 128, 128), BF16),
            pltpu.VMEM((n_f, 128, 128), BF16),
            pltpu.VMEM((n_f, 128, 128), BF16),
            pltpu.VMEM((n_y, 128, 128), BF16),
            pltpu.VMEM((n_z, 128, 128), BF16),
            pltpu.VMEM((2, 128, 128), BF16),
            pltpu.VMEM((2, n_f, 64, 128), BF16),
            pltpu.VMEM((n_f, 64, 128), BF16),
            pltpu.VMEM((n_f, 64, 128), BF16),
            pltpu.VMEM((n_f, 64, 128), BF16),
            pltpu.VMEM((n_y, 64, 128), BF16),
            pltpu.VMEM((n_z, 64, 128), BF16),
            pltpu.VMEM((2, n_f, 64, 128), BF16),
            pltpu.SemaphoreType.DMA((N_SEMS,)),
            pltpu.SemaphoreType.DMA((N_SEMS,)),
        ],
        compiler_params=pltpu.CompilerParams(collective_id=0, has_side_effects=True),
        name="block",
    )(vol, cot, w1f, w1b, w2l)
    return (
        jnp.transpose(features, (1, 0, 2))[:, None],
        jnp.transpose(volume_grad, (2, 0, 1, 3)),
        first_grad,
        second_grad,
    )


def solution(mesh):
    n_s, n_f = mesh.shape["space"], mesh.shape["filt"]
    n_z = 4 if n_s % 8 == 0 else 1
    sizes = (n_s, n_f, n_s // (2 * n_z), n_z)
    placed = (
        P(None, "space", "filt", None),
        P(),
        P(None, "filt", None),
        P("filt", "space", None, None),
    )
    return jax.shard_map(
        functools.partial(local, sizes),
        mesh=mesh,
        in_specs=placed,
        out_specs=(
            P("filt", "space", None, None),
            P(None, "space", "filt", None),
            P(),
            P(None, "filt", None),
        ),
        check_vma=False,
    )
```

```python
import functools

import jax
import jax.numpy as jnp
from jax import lax
from jax.experimental import pallas as pl
from jax.experimental.pallas import tpu as pltpu
from jax.sharding import PartitionSpec as P

MESH = pl.DeviceIdType.MESH
F32 = jnp.float32
BF16 = jnp.bfloat16
DIRS = [(dx, dy) for dx in (-1, 0, 1) for dy in (-1, 0, 1) if (dx, dy) != (0, 0)]
N_SEMS = 128


def sigmoid(v):
    return 1.0 / (1.0 + jnp.exp(-v))


def shifted(values, by):
    if by == 0:
        return values
    length = values.shape[1]
    lane = lax.broadcasted_iota(jnp.int32, values.shape, 1)
    if by == 1:
        return jnp.where(lane == length - 1, 0.0, pltpu.roll(values, length - 1, 1))
    return jnp.where(lane == 0, 0.0, pltpu.roll(values, 1, 1))


def nt_dot(a, b):
    return lax.dot_general(a, b, (((1,), (1,)), ((), ())), preferred_element_type=F32)


def side_by_side(left, right):
    return jnp.concatenate([left, right], axis=1)


def kernel(
    sizes,
    vol_hbm,
    cot_hbm,
    w1_hbm,
    w2_hbm,
    feat_out,
    vgrad_out,
    ag_out,
    os_out,
    vraw,
    craw,
    w1raw,
    w2raw,
    vrows,
    crows,
    cotb,
    w1f,
    w1b,
    w2p,
    ext,
    extd,
    slope1,
    cotg,
    w2g,
    w2t,
    ps,
    give,
    take,
    featb,
    s_gb,
    s_cb,
    s_pb,
    s_fb,
    s_yr,
    s_zr,
    s_os,
    f_gb,
    f_cb,
    f_pb,
    f_fb,
    f_yr,
    f_zr,
    f_ag,
    load_sem,
    send_sem,
    recv_sem,
):
    n_s, n_f, n_y, n_z = sizes
    s = lax.axis_index("space")
    f = lax.axis_index("filt")
    core = lax.rem(s, 2)
    zh = lax.rem(s // 2, n_z)
    y = s // (2 * n_z)

    loads = []
    for at, (whole, raw) in enumerate(
        ((vol_hbm, vraw), (w2_hbm, w2raw), (cot_hbm, craw), (w1_hbm, w1raw))
    ):
        load = pltpu.make_async_copy(whole, raw, load_sem.at[at])
        load.start()
        loads.append(load)

    def near(dx, dy):
        return (lax.rem(s + dx + n_s, n_s), lax.rem(f + dy + n_f, n_f))

    def along_f(j):
        return (s, lax.rem(f + j, n_f))

    def along_y(j):
        return ((lax.rem(y + j, n_y) * n_z + zh) * 2 + core, f)

    def along_z(j):
        return ((y * n_z + lax.rem(zh + j, n_z)) * 2 + core, f)

    twin = (s + 1 - 2 * core, f)

    peers = [near(dx, dy) for dx, dy in DIRS]
    peers += [along_f(j) for j in range(1, n_f)]
    peers += [along_y(j) for j in range(1, n_y)]
    peers += [along_z(j) for j in range(1, n_z)]
    peers += [twin]
    barrier = pltpu.get_barrier_semaphore()
    for peer in peers:
        pl.semaphore_signal(barrier, inc=1, device_id=peer, device_id_type=MESH)

    loads[0].wait()
    for c in range(64):
        for a in range(2):
            for h in range(2):
                vrows[h, 4 * c + 2 * a : 4 * c + 2 * a + 2] = vraw[
                    c, a, :, 128 * h : 128 * h + 128
                ].astype(F32)
    for a in range(2):
        for b in range(2):
            for h in range(2):
                ext[a + 1, b + 1, :, 128 * h : 128 * h + 128] = vrows[
                    h, pl.ds(2 * a + b, 64, stride=4), :
                ].astype(BF16)
    pl.semaphore_wait(barrier, len(peers))

    sent = []

    def send(src, dst, device):
        at = len(sent)
        copy = pltpu.make_async_remote_copy(
            src_ref=src,
            dst_ref=dst,
            send_sem=send_sem.at[at],
            recv_sem=recv_sem.at[at],
            device_id=device,
            device_id_type=MESH,
        )
        copy.start()
        sent.append(copy)
        return at

    def arrive(ref, at):
        pltpu.make_async_copy(ref, ref, recv_sem.at[at]).wait()

    def src_part(d):
        return {1: 2, -1: 1, 0: slice(1, 3)}[d]

    def dst_part(d):
        return {1: 0, -1: 3, 0: slice(1, 3)}[d]

    def halo_start(field):
        out = []
        for dx, dy in DIRS:
            target = field.at[dst_part(dx), dst_part(dy)]
            source = field.at[src_part(dx), src_part(dy)]
            out.append((send(source, target, near(dx, dy)), target))
        return out

    def finish(waits):
        for at, ref in waits:
            arrive(ref, at)

    def zero_rim(field, last):
        @pl.when(s == 0)
        def _():
            for b in range(last + 1):
                field[0, b] = jnp.zeros(field.shape[2:], field.dtype)

        @pl.when(s == n_s - 1)
        def _():
            for b in range(last + 1):
                field[last, b] = jnp.zeros(field.shape[2:], field.dtype)

        @pl.when(f == 0)
        def _():
            for a in range(last + 1):
                field[a, 0] = jnp.zeros(field.shape[2:], field.dtype)

        @pl.when(f == n_f - 1)
        def _():
            for a in range(last + 1):
                field[a, last] = jnp.zeros(field.shape[2:], field.dtype)

    vol_waits = halo_start(ext)

    loads[1].wait()
    for k in range(15):
        dz, c = k // 5, k % 5
        right = w2raw[6 * c + 3 + dz] if c < 4 else jnp.zeros((16, 64), BF16)
        w2p[k] = side_by_side(w2raw[6 * c + dz], right)
    w2p[15] = jnp.zeros((16, 128), BF16)
    half = w2p.at[pl.ds(8 * core, 8)]
    w2_waits = []
    for j in range(1, n_f):
        source = lax.rem(f - j + n_f, n_f)
        w2_waits.append((send(half, w2g.at[core, f], along_f(j)), w2g.at[core, source]))
    w2g[core, f] = w2p[pl.ds(8 * core, 8)]

    loads[2].wait()
    crows[...] = craw[...].reshape(16 * n_f, 128).astype(F32)
    for k in range(n_f):
        cotb[k] = crows[pl.ds(k, 16, stride=n_f), :].astype(BF16)
    cot_waits = []
    for j in range(1, n_f):
        other = lax.rem(f + j, n_f)
        source = lax.rem(f - j + n_f, n_f)
        cot_waits.append((send(cotb.at[other], cotg.at[f], along_f(j)), cotg.at[source]))
    cotg[f] = cotb[f]

    loads[3].wait()
    for k in range(15):
        dz, c = k // 5, k % 5
        rows = slice(64 * dz, 64 * dz + 64)
        cols = slice(128 * c, 128 * c + 128)
        right = w1raw[6 * c + 3 + dz] if c < 4 else jnp.zeros((64, 64), BF16)
        w1f[rows, cols] = side_by_side(w1raw[6 * c + dz], right)
        back = [w1raw[3 * (8 - 2 * c) + dz]]
        back.append(w1raw[3 * (7 - 2 * c) + dz] if c < 4 else jnp.zeros((64, 64), BF16))
        w1b[rows, cols] = jnp.concatenate(back, axis=0).astype(F32).T.astype(BF16)
    ps[3, 0] = jnp.zeros((64, 128), BF16)
    pair_row = lax.broadcasted_iota(jnp.int32, (256, 128), 0)
    pair_col = lax.broadcasted_iota(jnp.int32, (256, 128), 1)
    below = pair_row - 2 * pair_col
    pairs = jnp.where((below == 0) | (below == 1), 1.0, 0.0).astype(BF16)

    def stack(field, a, b):
        planes = [field[a + i, b + j] for i in range(3) for j in range(3)]
        return jnp.concatenate(planes + [jnp.zeros((64, 256), BF16)], axis=0)

    finish(vol_waits)
    zero_rim(ext, 3)

    wf = w1f[...]
    total = jnp.zeros((64, 128), F32)
    for a in range(2):
        for b in range(2):
            rows = jnp.dot(wf, stack(ext, a, b), preferred_element_type=F32)
            pre = shifted(rows[0:64], -1) + rows[64:128] + shifted(rows[128:192], 1)
            gate = sigmoid(pre)
            slope1[a, b] = gate * (1.0 + pre * (1.0 - gate))
            hidden = (pre * gate).astype(BF16)
            total = total + jnp.dot(hidden, pairs, preferred_element_type=F32)
    ps[1, 1] = (0.125 * total).astype(BF16)

    pool_waits = []
    for dx, dy in DIRS:
        target = ps.at[1 - dx, 1 - dy]
        pool_waits.append((send(ps.at[1, 1], target, near(dx, dy)), target))

    finish(w2_waits)
    w2_waits = [(send(w2g.at[core], w2g.at[core], twin), w2g.at[1 - core])]
    finish(cot_waits)
    finish(w2_waits)
    w2 = []
    for dz in range(3):
        tiles = [
            w2g[k // 8, :, k % 8].reshape(16 * n_f, 128) for k in range(5 * dz, 5 * dz + 5)
        ]
        w2.append(jnp.concatenate(tiles, axis=1))
        for c in range(5):
            w2t[dz, 128 * c : 128 * c + 128] = tiles[c].astype(F32).T.astype(BF16)

    finish(pool_waits)
    zero_rim(ps, 2)

    around = jnp.concatenate(
        [ps[i, j] for i in range(3) for j in range(3)] + [ps[3, 0]], axis=0
    )
    rows = [jnp.dot(w, around, preferred_element_type=F32) for w in w2]
    pre = shifted(rows[0], -1) + rows[1] + shifted(rows[2], 1)
    gate = sigmoid(pre)
    down = cotg[...].reshape(128, 128).astype(F32) * (gate * (1.0 + pre * (1.0 - gate)))
    down_own = down.astype(BF16)

    rows = [jnp.dot(w2t[dz], down_own, preferred_element_type=F32) for dz in range(3)]
    share = shifted(rows[0], 1) + rows[1] + shifted(rows[2], -1)
    down_waits = []
    for dx, dy in DIRS:
        slot = 3 * (dx + 1) + dy + 1
        give[slot] = share[64 * slot : 64 * slot + 64].astype(BF16)
        target = take.at[1 - dx, 1 - dy]
        down_waits.append((send(give.at[slot], target, near(dx, dy)), target))
    own_share = share[256:320]
    featb[0] = (pre * gate).astype(BF16).reshape(n_f, 16, 128)

    feat_waits = []
    for j in range(1, n_f):
        other = lax.rem(f + j, n_f)
        source = lax.rem(f - j + n_f, n_f)
        feat_waits.append(
            (send(featb.at[0, other], featb.at[1, f], along_f(j)), featb.at[1, source])
        )
    featb[1, f] = featb[0, f]

    lhs = jnp.concatenate(
        [shifted(down, 1).astype(BF16), down_own, shifted(down, -1).astype(BF16)], axis=0
    )
    terms = nt_dot(lhs, around)

    def deal(values, height, buffer, per, step):
        for g in range(n_f):
            tiles = [
                values[per * g + step * r : per * g + step * r + height, 128 * c : 128 * c + 128]
                for r in range(3)
                for c in range(5)
            ]
            tiles.append(jnp.zeros((height, 128), F32))
            for half in range(2):
                piece = jnp.concatenate(tiles[8 * half : 8 * half + 8], axis=0)
                buffer[half, g] = piece.astype(BF16)

    deal(terms, 16, s_gb, 16, 128)

    def to_twin(gb, cb):
        return [(send(gb.at[1 - core], cb, twin), cb)]

    def over_filt(gb, cb, pb, fb):
        pb[...] = (gb[core].astype(F32) + cb[...].astype(F32)).astype(BF16)
        fb[f] = pb[f]
        waits = []
        for j in range(1, n_f):
            other = lax.rem(f + j, n_f)
            source = lax.rem(f - j + n_f, n_f)
            waits.append((send(pb.at[other], fb.at[f], along_f(j)), fb.at[source]))
        return waits

    def summed(ref, count):
        value = ref[0].astype(F32)
        for k in range(1, count):
            value = value + ref[k].astype(F32)
        return value.astype(BF16)

    def over_y(fb, yr):
        yr[y] = summed(fb, n_f)
        waits = []
        for j in range(1, n_y):
            source = lax.rem(y - j + n_y, n_y)
            waits.append((send(yr.at[y], yr.at[y], along_y(j)), yr.at[source]))
        return waits

    def over_z(yr, zr):
        zr[zh] = summed(yr, n_y)
        waits = []
        for j in range(1, n_z):
            source = lax.rem(zh - j + n_z, n_z)
            waits.append((send(zr.at[zh], zr.at[zh], along_z(j)), zr.at[source]))
        return waits

    s_waits = to_twin(s_gb, s_cb)

    finish(s_waits)
    s_waits = over_filt(s_gb, s_cb, s_pb, s_fb)

    finish(down_waits)
    zero_rim(take, 2)
    pool_grad = own_share
    for dx, dy in DIRS:
        pool_grad = pool_grad + take[1 - dx, 1 - dy].astype(F32)
    pool_grad = 0.125 * pool_grad
    high = pool_grad.astype(BF16)
    low = (pool_grad - high.astype(F32)).astype(BF16)
    spread = nt_dot(jnp.concatenate([high, low], axis=0), pairs)
    spread = spread[0:64] + spread[64:128]
    for a in range(2):
        for b in range(2):
            extd[a + 1, b + 1] = (spread * slope1[a, b]).astype(BF16)
    fd_waits = halo_start(extd)

    terms = jnp.zeros((192, 640), F32)
    for a in range(2):
        for b in range(2):
            own = extd[a + 1, b + 1]
            wide = own.astype(F32)
            lhs = jnp.concatenate(
                [shifted(wide, 1).astype(BF16), own, shifted(wide, -1).astype(BF16)], axis=0
            )
            terms = terms + nt_dot(lhs, stack(ext, a, b))
    deal(terms, 8, f_gb, 24, 8)
    f_waits = to_twin(f_gb, f_cb)

    finish(s_waits)
    s_waits = over_y(s_fb, s_yr)
    finish(f_waits)
    f_waits = over_filt(f_gb, f_cb, f_pb, f_fb)
    finish(s_waits)
    s_waits = over_z(s_yr, s_zr)

    finish(fd_waits)
    zero_rim(extd, 3)
    wb = w1b[...]
    for a in range(2):
        for b in range(2):
            rows = jnp.dot(wb, stack(extd, a, b), preferred_element_type=F32)
            plane = shifted(rows[0:64], 1) + rows[64:128] + shifted(rows[128:192], -1)
            for h in range(2):
                vrows[h, pl.ds(2 * a + b, 64, stride=4), :] = plane[:, 128 * h : 128 * h + 128]

    finish(f_waits)
    f_waits = over_y(f_fb, f_yr)

    for c in range(64):
        for a in range(2):
            for h in range(2):
                vgrad_out[c, a, :, 128 * h : 128 * h + 128] = vrows[
                    h, 4 * c + 2 * a : 4 * c + 2 * a + 2
                ].astype(BF16)

    finish(f_waits)
    f_waits = over_z(f_yr, f_zr)

    finish(s_waits)
    s_os[core] = summed(s_zr, n_z)
    s_waits = [(send(s_os.at[core], s_os.at[core], twin), s_os.at[1 - core])]
    finish(feat_waits)
    for k in range(n_f):
        crows[pl.ds(k, 16, stride=n_f), :] = featb[1, k].astype(F32)
    feat_out[...] = crows[...].reshape(16, 1, n_f, 128).astype(BF16)
    finish(s_waits)
    os_out[...] = s_os[...]

    finish(f_waits)
    f_ag[core, f] = summed(f_zr, n_z)
    f_waits = []
    for j in range(1, n_f):
        source = lax.rem(f - j + n_f, n_f)
        f_waits.append((send(f_ag.at[core, f], f_ag.at[core, f], along_f(j)), f_ag.at[core, source]))
    finish(f_waits)
    f_waits = [(send(f_ag.at[core], f_ag.at[core], twin), f_ag.at[1 - core])]
    finish(f_waits)
    ag_out[...] = f_ag[...]

    for copy in sent:
        copy.wait_send()


def unpack(n_f, scales, feat_in, vgrad_in, ag_in, os_in, feat_out, vgrad_out, g1_out, g2_out):
    fine_scale, bottom_scale = scales
    feat_out[...] = feat_in[...]
    vgrad_out[...] = vgrad_in[...]
    for k in range(15):
        dz, c = k // 5, k % 5
        tile = os_in[k // 8, 16 * (k % 8) : 16 * (k % 8) + 16].astype(F32) * bottom_scale
        g2_out[6 * c + dz] = tile[:, 0:64]
        if c < 4:
            g2_out[6 * c + 3 + dz] = pltpu.roll(tile, 64, 1)[:, 0:64]
    for g in range(n_f):
        both = [ag_in[h, g].astype(F32) * fine_scale for h in range(2)]
        for k in range(15):
            row = 24 * g + 8 * (k // 5)
            dz, o = row // 64, row % 64
            c = k % 5
            tile = both[k // 8][8 * (k % 8) : 8 * (k % 8) + 8]
            g1_out[6 * c + dz, o : o + 8] = tile[:, 0:64]
            if c < 4:
                g1_out[6 * c + 3 + dz, o : o + 8] = pltpu.roll(tile, 64, 1)[:, 0:64]


def local(sizes, volume, first_weight, second_weight, cotangent):
    n_s, n_f, n_y, n_z = sizes
    scales = (
        1.0 / float(n_s * 2 * n_f * 2 * 256) ** 0.5,
        1.0 / float(n_s * n_f * 128) ** 0.5,
    )
    vmem = pl.BlockSpec(memory_space=pltpu.VMEM)
    whole = pl.BlockSpec(memory_space=pltpu.HBM)
    operands = (volume, cotangent, first_weight, second_weight)
    shape = jax.ShapeDtypeStruct
    features, volume_grad, fine, bottom = pl.pallas_call(
        functools.partial(kernel, sizes),
        out_shape=(
            shape((16, 1, n_f, 128), BF16),
            shape((64, 2, 2, 256), BF16),
            shape((2, n_f, 64, 128), BF16),
            shape((2, 128, 128), BF16),
        ),
        in_specs=[whole] * 4,
        out_specs=(vmem,) * 4,
        scratch_shapes=[
            pltpu.VMEM((64, 2, 2, 256), BF16),
            pltpu.VMEM((16, 1, n_f, 128), BF16),
            pltpu.VMEM((27, 64, 64), BF16),
            pltpu.VMEM((27, 16, 64), BF16),
            pltpu.VMEM((2, 256, 128), F32),
            pltpu.VMEM((16 * n_f, 128), F32),
            pltpu.VMEM((n_f, 16, 128), BF16),
            pltpu.VMEM((192, 640), BF16),
            pltpu.VMEM((192, 640), BF16),
            pltpu.VMEM((16, 16, 128), BF16),
            pltpu.VMEM((4, 4, 64, 256), BF16),
            pltpu.VMEM((4, 4, 64, 256), BF16),
            pltpu.VMEM((2, 2, 64, 256), F32),
            pltpu.VMEM((n_f, 16, 128), BF16),
            pltpu.VMEM((2, n_f, 8, 16, 128), BF16),
            pltpu.VMEM((3, 640, 128), BF16),
            pltpu.VMEM((4, 3, 64, 128), BF16),
            pltpu.VMEM((9, 64, 128), BF16),
            pltpu.VMEM((3, 3, 64, 128), BF16),
            pltpu.VMEM((2, n_f, 16, 128), BF16),
            pltpu.VMEM((2, n_f, 128, 128), BF16),
            pltpu.VMEM((n_f, 128, 128), BF16),
            pltpu.VMEM((n_f, 128, 128), BF16),
            pltpu.VMEM((n_f, 128, 128), BF16),
            pltpu.VMEM((n_y, 128, 128), BF16),
            pltpu.VMEM((n_z, 128, 128), BF16),
            pltpu.VMEM((2, 128, 128), BF16),
            pltpu.VMEM((2, n_f, 64, 128), BF16),
            pltpu.VMEM((n_f, 64, 128), BF16),
            pltpu.VMEM((n_f, 64, 128), BF16),
            pltpu.VMEM((n_f, 64, 128), BF16),
            pltpu.VMEM((n_y, 64, 128), BF16),
            pltpu.VMEM((n_z, 64, 128), BF16),
            pltpu.VMEM((2, n_f, 64, 128), BF16),
            pltpu.SemaphoreType.DMA((4,)),
            pltpu.SemaphoreType.DMA((N_SEMS,)),
            pltpu.SemaphoreType.DMA((N_SEMS,)),
        ],
        compiler_params=pltpu.CompilerParams(
            collective_id=0, has_side_effects=True, vmem_limit_bytes=24 * 1024 * 1024
        ),
        name="block",
    )(*(pltpu.with_memory_space_constraint(v, pltpu.HBM) for v in operands))
    return pl.pallas_call(
        functools.partial(unpack, n_f, scales),
        out_shape=(
            shape((16, 1, n_f, 128), BF16),
            shape((64, 2, 2, 256), BF16),
            shape((27, 64, 64), F32),
            shape((27, 16, 64), F32),
        ),
        in_specs=[vmem] * 4,
        out_specs=(vmem,) * 4,
        compiler_params=pltpu.CompilerParams(vmem_limit_bytes=24 * 1024 * 1024),
        name="unpack",
    )(features, volume_grad, fine, bottom)


def solution(mesh):
    n_s, n_f = mesh.shape["space"], mesh.shape["filt"]
    n_z = 4 if n_s % 8 == 0 else 1
    sizes = (n_s, n_f, n_s // (2 * n_z), n_z)
    placed = (
        P(None, "space", "filt", None),
        P(),
        P(None, "filt", None),
        P("filt", "space", None, None),
    )
    return jax.shard_map(
        functools.partial(local, sizes),
        mesh=mesh,
        in_specs=placed,
        out_specs=(
            P("filt", "space", None, None),
            P(None, "space", "filt", None),
            P(),
            P(None, "filt", None),
        ),
        check_vma=False,
    )
```

```python
import functools

import jax
import jax.numpy as jnp
from jax import lax
from jax.experimental import pallas as pl
from jax.experimental.pallas import tpu as pltpu
from jax.sharding import PartitionSpec as P

MESH = pl.DeviceIdType.MESH
F32 = jnp.float32
BF16 = jnp.bfloat16
DIRS = [(-1, -1), (-1, 1), (1, -1), (1, 1), (-1, 0), (1, 0), (0, -1), (0, 1)]
N_SEMS = 108


def sigmoid(v):
    return 1.0 / (1.0 + jnp.exp(-v))


def shifted(values, by):
    if by == 0:
        return values
    length = values.shape[1]
    lane = lax.broadcasted_iota(jnp.int32, values.shape, 1)
    if by == 1:
        return jnp.where(lane == length - 1, 0.0, pltpu.roll(values, length - 1, 1))
    return jnp.where(lane == 0, 0.0, pltpu.roll(values, 1, 1))


def nt_dot(a, b):
    return lax.dot_general(a, b, (((1,), (1,)), ((), ())), preferred_element_type=F32)


def side_by_side(left, right):
    return jnp.concatenate([left, right], axis=1)


def kernel(
    sizes,
    vol_hbm,
    cot_hbm,
    w1_hbm,
    w2_hbm,
    feat_out,
    vgrad_out,
    ag_out,
    os_out,
    vraw,
    craw,
    w1raw,
    w2raw,
    vrows,
    crows,
    cotb,
    w1f,
    w1b,
    w2p,
    ext,
    extd,
    slope1,
    cotg,
    w2g,
    w2t,
    ps,
    give,
    take,
    featb,
    s_gb,
    s_cb,
    s_pb,
    s_fb,
    s_yr,
    s_zr,
    s_os,
    f_gb,
    f_cb,
    f_pb,
    f_xr,
    f_zr,
    f_ag,
    load_sem,
    send_sem,
    recv_sem,
):
    n_s, n_f, n_y, n_z = sizes
    s = lax.axis_index("space")
    f = lax.axis_index("filt")
    core = lax.rem(s, 2)
    zh = lax.rem(s // 2, n_z)
    y = s // (2 * n_z)

    loads = []
    for at, (whole, raw) in enumerate(
        ((vol_hbm, vraw), (w2_hbm, w2raw), (cot_hbm, craw), (w1_hbm, w1raw))
    ):
        load = pltpu.make_async_copy(whole, raw, load_sem.at[at])
        load.start()
        loads.append(load)

    def near(dx, dy):
        return (lax.rem(s + dx + n_s, n_s), lax.rem(f + dy + n_f, n_f))

    def along_f(j):
        return (s, lax.rem(f + j, n_f))

    def along_y(j):
        return ((lax.rem(y + j, n_y) * n_z + zh) * 2 + core, f)

    def along_z(j):
        return ((y * n_z + lax.rem(zh + j, n_z)) * 2 + core, f)

    twin = (s + 1 - 2 * core, f)
    n_x = n_f // 2
    n_xy = n_x * n_y
    x, zl = lax.rem(f, n_x), f // n_x
    at_xy = y * n_x + x
    at_z = 2 * zh + zl

    def over_plane(j):
        to = lax.rem(at_xy + j, n_xy)
        return ((to // n_x * n_z + zh) * 2 + core, zl * n_x + lax.rem(to, n_x))

    def over_depth(j):
        to = lax.rem(at_z + j, 2 * n_z)
        return ((y * n_z + to // 2) * 2 + core, lax.rem(to, 2) * n_x + x)

    to_f = [along_f(j) for j in range(1, n_f)]
    to_y = [along_y(j) for j in range(1, n_y)]
    to_z = [along_z(j) for j in range(1, n_z)]
    to_plane = [over_plane(j) for j in range(1, n_xy)]
    to_depth = [over_depth(j) for j in range(1, 2 * n_z)]

    def ahead(me, count):
        return [lax.rem(me + j, count) for j in range(1, count)]

    def behind(me, count):
        return [lax.rem(me - j + count, count) for j in range(1, count)]

    f_ahead, f_behind = ahead(f, n_f), behind(f, n_f)
    y_behind, z_behind = behind(y, n_y), behind(zh, n_z)
    plane_ahead, plane_behind = ahead(at_xy, n_xy), behind(at_xy, n_xy)
    depth_behind = behind(at_z, 2 * n_z)
    first, second = core == 0, core == 1

    peers = [near(dx, dy) for dx, dy in DIRS] + to_f + to_plane + to_depth
    barrier = pltpu.get_barrier_semaphore()
    for peer in peers:
        pl.semaphore_signal(barrier, inc=1, device_id=peer, device_id_type=MESH)

    loads[0].wait()
    for c in range(64):
        for a in range(2):
            for h in range(2):
                vrows[h, 4 * c + 2 * a : 4 * c + 2 * a + 2] = vraw[
                    c, a, :, 128 * h : 128 * h + 128
                ].astype(F32)
    for a in range(2):
        for b in range(2):
            for h in range(2):
                ext[a + 1, b + 1, :, 128 * h : 128 * h + 128] = vrows[
                    h, pl.ds(2 * a + b, 64, stride=4), :
                ].astype(BF16)
    pl.semaphore_wait(barrier, len(peers))

    sent = []
    groups = {}

    def send(src, dst, device, only=None, size=None):
        at = len(sent)
        groups.setdefault(only, []).append((at, size or (lambda: src)))
        copy = pltpu.make_async_remote_copy(
            src_ref=src,
            dst_ref=dst,
            send_sem=send_sem.at[at],
            recv_sem=recv_sem.at[at],
            device_id=device,
            device_id_type=MESH,
        )
        copy.start()
        sent.append(copy)
        return at

    def arrive(ref, at):
        ref = ref() if callable(ref) else ref
        pltpu.make_async_copy(ref, ref, recv_sem.at[at]).wait()

    def drain(only):
        for at, size in groups[only]:
            ref = size()
            pltpu.make_async_copy(ref, ref, send_sem.at[at]).wait()

    def src_part(d):
        return {1: 2, -1: 1, 0: slice(1, 3)}[d]

    def dst_part(d):
        return {1: 0, -1: 3, 0: slice(1, 3)}[d]

    def halo_start(field):
        out = []
        for dx, dy in DIRS:
            target = field.at[dst_part(dx), dst_part(dy)]
            source = field.at[src_part(dx), src_part(dy)]
            out.append((send(source, target, near(dx, dy)), target))
        return out

    def finish(waits):
        for at, ref in waits:
            arrive(ref, at)

    def zero_rim(field, last):
        @pl.when(s == 0)
        def _():
            for b in range(last + 1):
                field[0, b] = jnp.zeros(field.shape[2:], field.dtype)

        @pl.when(s == n_s - 1)
        def _():
            for b in range(last + 1):
                field[last, b] = jnp.zeros(field.shape[2:], field.dtype)

        @pl.when(f == 0)
        def _():
            for a in range(last + 1):
                field[a, 0] = jnp.zeros(field.shape[2:], field.dtype)

        @pl.when(f == n_f - 1)
        def _():
            for a in range(last + 1):
                field[a, last] = jnp.zeros(field.shape[2:], field.dtype)

    vol_waits = halo_start(ext)

    loads[1].wait()
    for k in range(15):
        dz, c = k // 5, k % 5
        right = w2raw[6 * c + 3 + dz] if c < 4 else jnp.zeros((16, 64), BF16)
        w2p[k] = side_by_side(w2raw[6 * c + dz], right)
    w2p[15] = jnp.zeros((16, 128), BF16)
    half = w2p.at[pl.ds(8 * core, 8)]
    w2_waits = []
    for j in range(1, n_f):
        source = lax.rem(f - j + n_f, n_f)
        w2_waits.append((send(half, w2g.at[core, f], along_f(j)), w2g.at[core, source]))
    w2g[core, f] = w2p[pl.ds(8 * core, 8)]

    loads[2].wait()
    crows[...] = craw[...].reshape(16 * n_f, 128).astype(F32)
    for k in range(n_f):
        cotb[k] = crows[pl.ds(k, 16, stride=n_f), :].astype(BF16)
    cot_waits = []
    for j in range(1, n_f):
        other = lax.rem(f + j, n_f)
        source = lax.rem(f - j + n_f, n_f)
        cot_waits.append((send(cotb.at[other], cotg.at[f], along_f(j)), cotg.at[source]))
    cotg[f] = cotb[f]

    loads[3].wait()
    for k in range(15):
        dz, c = k // 5, k % 5
        rows = slice(64 * dz, 64 * dz + 64)
        cols = slice(128 * c, 128 * c + 128)
        right = w1raw[6 * c + 3 + dz] if c < 4 else jnp.zeros((64, 64), BF16)
        w1f[rows, cols] = side_by_side(w1raw[6 * c + dz], right)
        back = [w1raw[3 * (8 - 2 * c) + dz]]
        back.append(w1raw[3 * (7 - 2 * c) + dz] if c < 4 else jnp.zeros((64, 64), BF16))
        w1b[rows, cols] = jnp.concatenate(back, axis=0).astype(F32).T.astype(BF16)
    ps[3, 0] = jnp.zeros((64, 128), BF16)
    pair_row = lax.broadcasted_iota(jnp.int32, (256, 128), 0)
    pair_col = lax.broadcasted_iota(jnp.int32, (256, 128), 1)
    below = pair_row - 2 * pair_col
    pairs = jnp.where((below == 0) | (below == 1), 1.0, 0.0).astype(BF16)

    def stack(field, a, b):
        planes = [field[a + i, b + j] for i in range(3) for j in range(3)]
        return jnp.concatenate(planes + [jnp.zeros((64, 256), BF16)], axis=0)

    finish(vol_waits)
    zero_rim(ext, 3)

    wf = w1f[...]
    total = jnp.zeros((64, 128), F32)
    for a in range(2):
        for b in range(2):
            rows = jnp.dot(wf, stack(ext, a, b), preferred_element_type=F32)
            pre = shifted(rows[0:64], -1) + rows[64:128] + shifted(rows[128:192], 1)
            gate = sigmoid(pre)
            slope1[a, b] = gate * (1.0 + pre * (1.0 - gate))
            hidden = (pre * gate).astype(BF16)
            total = total + jnp.dot(hidden, pairs, preferred_element_type=F32)
    ps[1, 1] = (0.125 * total).astype(BF16)

    pool_waits = []
    for dx, dy in DIRS:
        target = ps.at[1 - dx, 1 - dy]
        pool_waits.append((send(ps.at[1, 1], target, near(dx, dy)), target))

    finish(w2_waits)
    w2_waits = [(send(w2g.at[core], w2g.at[core], twin), w2g.at[1 - core])]
    finish(cot_waits)
    finish(w2_waits)
    w2 = []
    for dz in range(3):
        tiles = [
            w2g[k // 8, :, k % 8].reshape(16 * n_f, 128) for k in range(5 * dz, 5 * dz + 5)
        ]
        w2.append(jnp.concatenate(tiles, axis=1))
        for c in range(5):
            w2t[dz, 128 * c : 128 * c + 128] = tiles[c].astype(F32).T.astype(BF16)

    finish(pool_waits)
    zero_rim(ps, 2)

    around = jnp.concatenate(
        [ps[i, j] for i in range(3) for j in range(3)] + [ps[3, 0]], axis=0
    )
    rows = [jnp.dot(w, around, preferred_element_type=F32) for w in w2]
    pre = shifted(rows[0], -1) + rows[1] + shifted(rows[2], 1)
    gate = sigmoid(pre)
    down = cotg[...].reshape(128, 128).astype(F32) * (gate * (1.0 + pre * (1.0 - gate)))
    down_own = down.astype(BF16)

    rows = [jnp.dot(w2t[dz], down_own, preferred_element_type=F32) for dz in range(3)]
    share = shifted(rows[0], 1) + rows[1] + shifted(rows[2], -1)
    down_waits = []
    for dx, dy in DIRS:
        slot = 3 * (dx + 1) + dy + 1
        give[slot] = share[64 * slot : 64 * slot + 64].astype(BF16)
        target = take.at[1 - dx, 1 - dy]
        down_waits.append((send(give.at[slot], target, near(dx, dy)), target))
    own_share = share[256:320]
    featb[0] = (pre * gate).astype(BF16).reshape(n_f, 16, 128)

    feat_waits = []
    for j in range(1, n_f):
        other = lax.rem(f + j, n_f)
        source = lax.rem(f - j + n_f, n_f)
        feat_waits.append(
            (send(featb.at[0, other], featb.at[1, f], along_f(j)), featb.at[1, source])
        )
    featb[1, f] = featb[0, f]

    lhs = jnp.concatenate(
        [shifted(down, 1).astype(BF16), down_own, shifted(down, -1).astype(BF16)], axis=0
    )
    terms = nt_dot(lhs, around)

    def deal(values, height, per, step, put):
        for g in range(n_f):
            tiles = [
                values[per * g + step * r : per * g + step * r + height, 128 * c : 128 * c + 128]
                for r in range(3)
                for c in range(5)
            ]
            tiles.append(jnp.zeros((height, 128), F32))
            put(g, jnp.concatenate(tiles, axis=0).astype(BF16))

    def put_bottom(g, piece):
        s_gb[g] = piece

    deal(terms, 16, 16, 128, put_bottom)

    def exchange(ref, mine, peers, sources, only):
        return [
            (
                send(ref.at[mine], ref.at[mine], peer, only, lambda: ref.at[mine]),
                lambda source=source: ref.at[source],
            )
            for peer, source in zip(peers, sources)
        ]

    def scatter(out, into, mine, peers, theirs, sources, only):
        return [
            (
                send(out.at[other], into.at[mine], peer, only, lambda other=other: out.at[other]),
                lambda source=source: into.at[source],
            )
            for peer, other, source in zip(peers, theirs, sources)
        ]

    def summed(ref, count):
        value = ref[0].astype(F32)
        for k in range(1, count):
            value = value + ref[k].astype(F32)
        return value.astype(BF16)

    s_waits, f_waits = [], []

    @pl.when(second)
    def _():
        send(s_gb, s_cb, twin, 1)

    s_twin = len(sent) - 1

    @pl.when(first)
    def _():
        arrive(s_cb, s_twin)
        s_pb[...] = (s_gb[...].astype(F32) + s_cb[...].astype(F32)).astype(BF16)
        s_fb[f] = s_pb[f]
        s_waits.extend(scatter(s_pb, s_fb, f, to_f, f_ahead, f_behind, 0))

    finish(down_waits)
    zero_rim(take, 2)
    pool_grad = own_share
    for dx, dy in DIRS:
        pool_grad = pool_grad + take[1 - dx, 1 - dy].astype(F32)
    pool_grad = 0.125 * pool_grad
    high = pool_grad.astype(BF16)
    low = (pool_grad - high.astype(F32)).astype(BF16)
    spread = nt_dot(jnp.concatenate([high, low], axis=0), pairs)
    spread = spread[0:64] + spread[64:128]
    for a in range(2):
        for b in range(2):
            extd[a + 1, b + 1] = (spread * slope1[a, b]).astype(BF16)
    fd_waits = halo_start(extd)

    terms = jnp.zeros((192, 640), F32)
    for a in range(2):
        for b in range(2):
            own = extd[a + 1, b + 1]
            wide = own.astype(F32)
            lhs = jnp.concatenate(
                [shifted(wide, 1).astype(BF16), own, shifted(wide, -1).astype(BF16)], axis=0
            )
            terms = terms + nt_dot(lhs, stack(ext, a, b))

    per_peer = 16 // n_xy

    def put_fine(g, piece):
        for h in range(2):
            at = 2 * g + h
            row = 64 * (at % per_peer)
            f_gb[at // per_peer, row : row + 64] = piece[64 * h : 64 * h + 64]

    deal(terms, 8, 24, 8, put_fine)

    @pl.when(first)
    def _():
        send(f_gb, f_cb, twin, 0)

    f_twin = len(sent) - 1
    plane_waits, y_waits = [], []

    @pl.when(second)
    def _():
        arrive(f_cb, f_twin)
        f_pb[...] = (f_gb[...].astype(F32) + f_cb[...].astype(F32)).astype(BF16)
        f_xr[at_xy] = f_pb[at_xy]
        plane_waits.extend(
            scatter(f_pb, f_xr, at_xy, to_plane, plane_ahead, plane_behind, 1)
        )

    @pl.when(first)
    def _():
        finish(s_waits)
        s_yr[y] = summed(s_fb, n_f)
        y_waits.extend(exchange(s_yr, y, to_y, y_behind, 0))

    finish(fd_waits)
    zero_rim(extd, 3)
    wb = w1b[...]
    for a in range(2):
        for b in range(2):
            rows = jnp.dot(wb, stack(extd, a, b), preferred_element_type=F32)
            plane = shifted(rows[0:64], 1) + rows[64:128] + shifted(rows[128:192], -1)
            for h in range(2):
                vrows[h, pl.ds(2 * a + b, 64, stride=4), :] = plane[:, 128 * h : 128 * h + 128]

    for c in range(64):
        for a in range(2):
            for h in range(2):
                vgrad_out[c, a, :, 128 * h : 128 * h + 128] = vrows[
                    h, 4 * c + 2 * a : 4 * c + 2 * a + 2
                ].astype(BF16)

    depth_waits, z_waits = [], []

    @pl.when(second)
    def _():
        finish(plane_waits)
        f_zr[at_z] = summed(f_xr, n_xy)
        depth_waits.extend(exchange(f_zr, at_z, to_depth, depth_behind, 1))

    @pl.when(first)
    def _():
        finish(y_waits)
        s_zr[zh] = summed(s_yr, n_y)
        z_waits.extend(exchange(s_zr, zh, to_z, z_behind, 0))

    finish(feat_waits)
    for k in range(n_f):
        crows[pl.ds(k, 16, stride=n_f), :] = featb[1, k].astype(F32)
    feat_out[...] = crows[...].reshape(16, 1, n_f, 128).astype(BF16)

    @pl.when(first)
    def _():
        finish(z_waits)
        s_os[...] = summed(s_zr, n_z)
        send(s_os, s_os, twin, 0)

    s_last = len(sent) - 1

    @pl.when(second)
    def _():
        finish(depth_waits)
        f_ag[at_xy] = summed(f_zr, 2 * n_z)
        finish(exchange(f_ag, at_xy, to_plane, plane_behind, 1))
        send(f_ag, f_ag, twin, 1)
        arrive(s_os, s_last)

    f_last = len(sent) - 1

    @pl.when(first)
    def _():
        arrive(f_ag, f_last)

    os_out[...] = s_os[...]
    ag_out[...] = f_ag[...]

    assert len(sent) <= N_SEMS
    drain(None)

    @pl.when(first)
    def _():
        drain(0)

    @pl.when(second)
    def _():
        drain(1)


def unpack(n_f, scales, feat_in, vgrad_in, ag_in, os_in, feat_out, vgrad_out, g1_out, g2_out):
    fine_scale, bottom_scale = scales
    feat_out[...] = feat_in[...]
    vgrad_out[...] = vgrad_in[...]
    for k in range(15):
        dz, c = k // 5, k % 5
        tile = os_in[16 * k : 16 * k + 16].astype(F32) * bottom_scale
        g2_out[6 * c + dz] = tile[:, 0:64]
        if c < 4:
            g2_out[6 * c + 3 + dz] = pltpu.roll(tile, 64, 1)[:, 0:64]
    for g in range(n_f):
        per_peer = 16 // ag_in.shape[0]
        both = []
        for at in (2 * g, 2 * g + 1):
            start = 64 * (at % per_peer)
            both.append(ag_in[at // per_peer, start : start + 64].astype(F32) * fine_scale)
        for k in range(15):
            row = 24 * g + 8 * (k // 5)
            dz, o = row // 64, row % 64
            c = k % 5
            tile = both[k // 8][8 * (k % 8) : 8 * (k % 8) + 8]
            g1_out[6 * c + dz, o : o + 8] = tile[:, 0:64]
            if c < 4:
                g1_out[6 * c + 3 + dz, o : o + 8] = pltpu.roll(tile, 64, 1)[:, 0:64]


def local(sizes, volume, first_weight, second_weight, cotangent):
    n_s, n_f, n_y, n_z = sizes
    n_xy = n_f // 2 * n_y
    scales = (
        1.0 / float(n_s * 2 * n_f * 2 * 256) ** 0.5,
        1.0 / float(n_s * n_f * 128) ** 0.5,
    )
    vmem = pl.BlockSpec(memory_space=pltpu.VMEM)
    whole = pl.BlockSpec(memory_space=pltpu.HBM)
    operands = (volume, cotangent, first_weight, second_weight)
    shape = jax.ShapeDtypeStruct
    features, volume_grad, fine, bottom = pl.pallas_call(
        functools.partial(kernel, sizes),
        out_shape=(
            shape((16, 1, n_f, 128), BF16),
            shape((64, 2, 2, 256), BF16),
            shape((n_xy, 1024 // n_xy, 128), BF16),
            shape((256, 128), BF16),
        ),
        in_specs=[whole] * 4,
        out_specs=(vmem,) * 4,
        scratch_shapes=[
            pltpu.VMEM((64, 2, 2, 256), BF16),
            pltpu.VMEM((16, 1, n_f, 128), BF16),
            pltpu.VMEM((27, 64, 64), BF16),
            pltpu.VMEM((27, 16, 64), BF16),
            pltpu.VMEM((2, 256, 128), F32),
            pltpu.VMEM((16 * n_f, 128), F32),
            pltpu.VMEM((n_f, 16, 128), BF16),
            pltpu.VMEM((192, 640), BF16),
            pltpu.VMEM((192, 640), BF16),
            pltpu.VMEM((16, 16, 128), BF16),
            pltpu.VMEM((4, 4, 64, 256), BF16),
            pltpu.VMEM((4, 4, 64, 256), BF16),
            pltpu.VMEM((2, 2, 64, 256), F32),
            pltpu.VMEM((n_f, 16, 128), BF16),
            pltpu.VMEM((2, n_f, 8, 16, 128), BF16),
            pltpu.VMEM((3, 640, 128), BF16),
            pltpu.VMEM((4, 3, 64, 128), BF16),
            pltpu.VMEM((9, 64, 128), BF16),
            pltpu.VMEM((3, 3, 64, 128), BF16),
            pltpu.VMEM((2, n_f, 16, 128), BF16),
            pltpu.VMEM((n_f, 256, 128), BF16),
            pltpu.VMEM((n_f, 256, 128), BF16),
            pltpu.VMEM((n_f, 256, 128), BF16),
            pltpu.VMEM((n_f, 256, 128), BF16),
            pltpu.VMEM((n_y, 256, 128), BF16),
            pltpu.VMEM((n_z, 256, 128), BF16),
            pltpu.VMEM((256, 128), BF16),
            pltpu.VMEM((n_xy, 1024 // n_xy, 128), BF16),
            pltpu.VMEM((n_xy, 1024 // n_xy, 128), BF16),
            pltpu.VMEM((n_xy, 1024 // n_xy, 128), BF16),
            pltpu.VMEM((n_xy, 1024 // n_xy, 128), BF16),
            pltpu.VMEM((2 * n_z, 1024 // n_xy, 128), BF16),
            pltpu.VMEM((n_xy, 1024 // n_xy, 128), BF16),
            pltpu.SemaphoreType.DMA((4,)),
            pltpu.SemaphoreType.DMA((N_SEMS,)),
            pltpu.SemaphoreType.DMA((N_SEMS,)),
        ],
        compiler_params=pltpu.CompilerParams(
            collective_id=0, has_side_effects=True, vmem_limit_bytes=24 * 1024 * 1024
        ),
        name="block",
    )(*(pltpu.with_memory_space_constraint(v, pltpu.HBM) for v in operands))
    return pl.pallas_call(
        functools.partial(unpack, n_f, scales),
        out_shape=(
            shape((16, 1, n_f, 128), BF16),
            shape((64, 2, 2, 256), BF16),
            shape((27, 64, 64), F32),
            shape((27, 16, 64), F32),
        ),
        in_specs=[vmem] * 4,
        out_specs=(vmem,) * 4,
        compiler_params=pltpu.CompilerParams(vmem_limit_bytes=24 * 1024 * 1024),
        name="unpack",
    )(features, volume_grad, fine, bottom)


def solution(mesh):
    n_s, n_f = mesh.shape["space"], mesh.shape["filt"]
    n_z = 4 if n_s % 8 == 0 else 1
    sizes = (n_s, n_f, n_s // (2 * n_z), n_z)
    placed = (
        P(None, "space", "filt", None),
        P(),
        P(None, "filt", None),
        P("filt", "space", None, None),
    )
    return jax.shard_map(
        functools.partial(local, sizes),
        mesh=mesh,
        in_specs=placed,
        out_specs=(
            P("filt", "space", None, None),
            P(None, "space", "filt", None),
            P(),
            P(None, "filt", None),
        ),
        check_vma=False,
    )
```

```python
import functools

import jax
import jax.numpy as jnp
from jax import lax
from jax.experimental import pallas as pl
from jax.experimental.pallas import tpu as pltpu
from jax.sharding import PartitionSpec as P

MESH = pl.DeviceIdType.MESH
F32 = jnp.float32
BF16 = jnp.bfloat16
DIRS = [(-1, -1), (-1, 1), (1, -1), (1, 1), (-1, 0), (1, 0), (0, -1), (0, 1)]
N_SEMS = 130


def sigmoid(v):
    return 1.0 / (1.0 + jnp.exp(-v))


def shifted(values, by):
    if by == 0:
        return values
    length = values.shape[1]
    lane = lax.broadcasted_iota(jnp.int32, values.shape, 1)
    if by == 1:
        return jnp.where(lane == length - 1, 0.0, pltpu.roll(values, length - 1, 1))
    return jnp.where(lane == 0, 0.0, pltpu.roll(values, 1, 1))


def nt_dot(a, b):
    return lax.dot_general(a, b, (((1,), (1,)), ((), ())), preferred_element_type=F32)


def side_by_side(left, right):
    return jnp.concatenate([left, right], axis=1)


def kernel(
    sizes,
    vol_hbm,
    cot_hbm,
    w1_hbm,
    w2_hbm,
    feat_out,
    vgrad_out,
    ag_out,
    os_out,
    vraw,
    craw,
    w1raw,
    w2raw,
    vrows,
    crows,
    cotb,
    w1f,
    w1b,
    w2p,
    ext,
    extd,
    slope1,
    cotg,
    w2g,
    w2t,
    ps,
    give,
    take,
    featb,
    s_gb,
    s_cb,
    s_pb,
    s_fb,
    s_yr,
    s_zr,
    s_os,
    f_gb,
    f_cb,
    f_pb,
    f_xr,
    f_zr,
    f_ag,
    load_sem,
    send_sem,
    recv_sem,
):
    n_s, n_f, n_y, n_z = sizes
    s = lax.axis_index("space")
    f = lax.axis_index("filt")
    core = lax.rem(s, 2)
    zh = lax.rem(s // 2, n_z)
    y = s // (2 * n_z)

    loads = []
    for at, (whole, raw) in enumerate(
        ((vol_hbm, vraw), (w2_hbm, w2raw), (cot_hbm, craw), (w1_hbm, w1raw))
    ):
        load = pltpu.make_async_copy(whole, raw, load_sem.at[at])
        load.start()
        loads.append(load)

    def near(dx, dy):
        return (lax.rem(s + dx + n_s, n_s), lax.rem(f + dy + n_f, n_f))

    def along_f(j):
        return (s, lax.rem(f + j, n_f))

    def along_y(j):
        return ((lax.rem(y + j, n_y) * n_z + zh) * 2 + core, f)

    def along_z(j):
        return ((y * n_z + lax.rem(zh + j, n_z)) * 2 + core, f)

    twin = (s + 1 - 2 * core, f)
    n_x = n_f // 2
    n_xy = n_x * n_y
    x, zl = lax.rem(f, n_x), f // n_x
    at_xy = y * n_x + x
    at_z = 2 * zh + zl

    def over_plane(j):
        to = lax.rem(at_xy + j, n_xy)
        return ((to // n_x * n_z + zh) * 2 + core, zl * n_x + lax.rem(to, n_x))

    def over_depth(j):
        to = lax.rem(at_z + j, 2 * n_z)
        return ((y * n_z + to // 2) * 2 + core, lax.rem(to, 2) * n_x + x)

    to_f = [along_f(j) for j in range(1, n_f)]
    to_y = [along_y(j) for j in range(1, n_y)]
    to_z = [along_z(j) for j in range(1, n_z)]
    to_plane = [over_plane(j) for j in range(1, n_xy)]
    to_depth = [over_depth(j) for j in range(1, 2 * n_z)]

    def ahead(me, count):
        return [lax.rem(me + j, count) for j in range(1, count)]

    def behind(me, count):
        return [lax.rem(me - j + count, count) for j in range(1, count)]

    f_ahead, f_behind = ahead(f, n_f), behind(f, n_f)
    y_behind, z_behind = behind(y, n_y), behind(zh, n_z)
    plane_ahead, plane_behind = ahead(at_xy, n_xy), behind(at_xy, n_xy)
    depth_behind = behind(at_z, 2 * n_z)
    first, second = core == 0, core == 1
    in_s = {-1: s > 0, 0: s >= 0, 1: s < n_s - 1}
    in_f = {-1: f > 0, 0: f >= 0, 1: f < n_f - 1}
    exists = {(dx, dy): in_s[dx] & in_f[dy] for dx, dy in DIRS}
    beside = {d: near(*d) for d in DIRS}
    flip = (1 - zl) * n_x + x
    x_ahead = [zl * n_x + lax.rem(x + j, n_x) for j in range(1, n_x)]
    x_behind = [lax.rem(x - j + n_x, n_x) for j in range(1, n_x)]

    peers = [beside[d] for d in DIRS] + to_f + to_plane + to_depth
    barrier = pltpu.get_barrier_semaphore()
    for peer in peers:
        pl.semaphore_signal(barrier, inc=1, device_id=peer, device_id_type=MESH)

    loads[0].wait()
    for c in range(64):
        for a in range(2):
            for h in range(2):
                vrows[h, 4 * c + 2 * a : 4 * c + 2 * a + 2] = vraw[
                    c, a, :, 128 * h : 128 * h + 128
                ].astype(F32)
    for a in range(2):
        for b in range(2):
            for h in range(2):
                ext[a + 1, b + 1, :, 128 * h : 128 * h + 128] = vrows[
                    h, pl.ds(2 * a + b, 64, stride=4), :
                ].astype(BF16)
    pl.semaphore_wait(barrier, len(peers))

    sent = []
    groups = {}

    def send(src, dst, device, only=None, size=None):
        at = len(sent)
        groups.setdefault(only, []).append((at, size or (lambda: src)))
        copy = pltpu.make_async_remote_copy(
            src_ref=src,
            dst_ref=dst,
            send_sem=send_sem.at[at],
            recv_sem=recv_sem.at[at],
            device_id=device,
            device_id_type=MESH,
        )
        copy.start()
        sent.append(copy)
        return at

    def arrive(ref, at):
        ref = ref() if callable(ref) else ref
        pltpu.make_async_copy(ref, ref, recv_sem.at[at]).wait()

    def drain(only):
        for at, size in groups[only]:
            ref = size()
            pltpu.make_async_copy(ref, ref, send_sem.at[at]).wait()

    def src_part(d):
        return {1: 2, -1: 1, 0: slice(1, 3)}[d]

    def dst_part(d):
        return {1: 0, -1: 3, 0: slice(1, 3)}[d]

    def halo_start(field):
        out = []
        for d in DIRS:
            dx, dy = d

            def source(dx=dx, dy=dy):
                return field.at[src_part(dx), src_part(dy)]

            def target(dx=dx, dy=dy):
                return field.at[dst_part(dx), dst_part(dy)]

            @pl.when(exists[d])
            def _(d=d, source=source, target=target):
                send(source(), target(), beside[d], d, source)

            out.append((d, len(sent) - 1, target))
        return out

    def halo_finish(waits):
        for (dx, dy), at, target in waits:

            @pl.when(exists[-dx, -dy])
            def _(at=at, target=target):
                arrive(target, at)

    def finish(waits):
        for at, ref in waits:
            arrive(ref, at)

    def zero_rim(field, last):
        @pl.when(s == 0)
        def _():
            for b in range(last + 1):
                field[0, b] = jnp.zeros(field.shape[2:], field.dtype)

        @pl.when(s == n_s - 1)
        def _():
            for b in range(last + 1):
                field[last, b] = jnp.zeros(field.shape[2:], field.dtype)

        @pl.when(f == 0)
        def _():
            for a in range(last + 1):
                field[a, 0] = jnp.zeros(field.shape[2:], field.dtype)

        @pl.when(f == n_f - 1)
        def _():
            for a in range(last + 1):
                field[a, last] = jnp.zeros(field.shape[2:], field.dtype)

    vol_waits = halo_start(ext)
    zero_rim(ext, 3)
    zero_rim(extd, 3)

    loads[1].wait()
    for k in range(15):
        dz, c = k // 5, k % 5
        right = w2raw[6 * c + 3 + dz] if c < 4 else jnp.zeros((16, 64), BF16)
        w2p[k] = side_by_side(w2raw[6 * c + dz], right)
    w2p[15] = jnp.zeros((16, 128), BF16)
    half = w2p.at[pl.ds(8 * core, 8)]
    w2_flip = send(half, w2g.at[core, f], (s, flip))
    w2_waits = []
    for j, to in enumerate(x_ahead):
        source = zl * n_x + x_behind[j]
        w2_waits.append((send(half, w2g.at[core, f], (s, to)), w2g.at[core, source]))
    w2g[core, f] = w2p[pl.ds(8 * core, 8)]

    loads[2].wait()
    crows[...] = craw[...].reshape(16 * n_f, 128).astype(F32)
    for k in range(n_f):
        cotb[k] = crows[pl.ds(k, 16, stride=n_f), :].astype(BF16)
    cot_waits = []
    for j in range(1, n_f):
        other = lax.rem(f + j, n_f)
        source = lax.rem(f - j + n_f, n_f)
        cot_waits.append((send(cotb.at[other], cotg.at[f], along_f(j)), cotg.at[source]))
    cotg[f] = cotb[f]

    loads[3].wait()
    for k in range(15):
        dz, c = k // 5, k % 5
        rows = slice(64 * dz, 64 * dz + 64)
        cols = slice(128 * c, 128 * c + 128)
        right = w1raw[6 * c + 3 + dz] if c < 4 else jnp.zeros((64, 64), BF16)
        w1f[rows, cols] = side_by_side(w1raw[6 * c + dz], right)
        back = [w1raw[3 * (8 - 2 * c) + dz]]
        back.append(w1raw[3 * (7 - 2 * c) + dz] if c < 4 else jnp.zeros((64, 64), BF16))
        w1b[rows, cols] = jnp.concatenate(back, axis=0).astype(F32).T.astype(BF16)
    ps[3, 0] = jnp.zeros((64, 128), BF16)
    pair_row = lax.broadcasted_iota(jnp.int32, (256, 128), 0)
    pair_col = lax.broadcasted_iota(jnp.int32, (256, 128), 1)
    below = pair_row - 2 * pair_col
    pairs = jnp.where((below == 0) | (below == 1), 1.0, 0.0).astype(BF16)

    def stack(field, a, b):
        planes = [field[a + i, b + j] for i in range(3) for j in range(3)]
        return jnp.concatenate(planes + [jnp.zeros((64, 256), BF16)], axis=0)

    arrive(w2g.at[core, flip], w2_flip)
    for j, to in enumerate(x_ahead):
        mine = w2g.at[core, flip]
        source = (1 - zl) * n_x + x_behind[j]
        w2_waits.append((send(mine, mine, (s, to)), w2g.at[core, source]))
    halo_finish(vol_waits)

    wf = w1f[...]
    total = jnp.zeros((64, 128), F32)
    for a in range(2):
        for b in range(2):
            rows = jnp.dot(wf, stack(ext, a, b), preferred_element_type=F32)
            pre = shifted(rows[0:64], -1) + rows[64:128] + shifted(rows[128:192], 1)
            gate = sigmoid(pre)
            slope1[a, b] = gate * (1.0 + pre * (1.0 - gate))
            hidden = (pre * gate).astype(BF16)
            total = total + jnp.dot(hidden, pairs, preferred_element_type=F32)
    ps[1, 1] = (0.125 * total).astype(BF16)

    pool_waits = []
    for dx, dy in DIRS:
        target = ps.at[1 - dx, 1 - dy]
        pool_waits.append((send(ps.at[1, 1], target, near(dx, dy)), target))

    finish(w2_waits)
    w2_waits = [(send(w2g.at[core], w2g.at[core], twin), w2g.at[1 - core])]
    finish(cot_waits)
    finish(w2_waits)
    w2 = []
    for dz in range(3):
        tiles = [
            w2g[k // 8, :, k % 8].reshape(16 * n_f, 128) for k in range(5 * dz, 5 * dz + 5)
        ]
        w2.append(jnp.concatenate(tiles, axis=1))
        for c in range(5):
            w2t[dz, 128 * c : 128 * c + 128] = tiles[c].astype(F32).T.astype(BF16)

    finish(pool_waits)
    zero_rim(ps, 2)

    around = jnp.concatenate(
        [ps[i, j] for i in range(3) for j in range(3)] + [ps[3, 0]], axis=0
    )
    rows = [jnp.dot(w, around, preferred_element_type=F32) for w in w2]
    pre = shifted(rows[0], -1) + rows[1] + shifted(rows[2], 1)
    gate = sigmoid(pre)
    down = cotg[...].reshape(128, 128).astype(F32) * (gate * (1.0 + pre * (1.0 - gate)))
    down_own = down.astype(BF16)

    rows = [jnp.dot(w2t[dz], down_own, preferred_element_type=F32) for dz in range(3)]
    share = shifted(rows[0], 1) + rows[1] + shifted(rows[2], -1)
    down_waits = []
    for dx, dy in DIRS:
        slot = 3 * (dx + 1) + dy + 1
        give[slot] = share[64 * slot : 64 * slot + 64].astype(BF16)
        target = take.at[1 - dx, 1 - dy]
        down_waits.append((send(give.at[slot], target, near(dx, dy)), target))
    own_share = share[256:320]
    featb[0] = (pre * gate).astype(BF16).reshape(n_f, 16, 128)

    feat_waits = []
    for j in range(1, n_f):
        other = lax.rem(f + j, n_f)
        source = lax.rem(f - j + n_f, n_f)
        feat_waits.append(
            (send(featb.at[0, other], featb.at[1, f], along_f(j)), featb.at[1, source])
        )
    featb[1, f] = featb[0, f]

    lhs = jnp.concatenate(
        [shifted(down, 1).astype(BF16), down_own, shifted(down, -1).astype(BF16)], axis=0
    )
    terms = nt_dot(lhs, around)

    def deal(values, height, per, step, put):
        for g in range(n_f):
            tiles = [
                values[per * g + step * r : per * g + step * r + height, 128 * c : 128 * c + 128]
                for r in range(3)
                for c in range(5)
            ]
            tiles.append(jnp.zeros((height, 128), F32))
            put(g, jnp.concatenate(tiles, axis=0).astype(BF16))

    def put_bottom(g, piece):
        s_gb[g] = piece

    deal(terms, 16, 16, 128, put_bottom)

    def exchange(ref, mine, peers, sources, only):
        return [
            (
                send(ref.at[mine], ref.at[mine], peer, only, lambda: ref.at[mine]),
                lambda source=source: ref.at[source],
            )
            for peer, source in zip(peers, sources)
        ]

    def scatter(out, into, mine, peers, theirs, sources, only):
        return [
            (
                send(out.at[other], into.at[mine], peer, only, lambda other=other: out.at[other]),
                lambda source=source: into.at[source],
            )
            for peer, other, source in zip(peers, theirs, sources)
        ]

    def summed(ref, count):
        value = ref[0].astype(F32)
        for k in range(1, count):
            value = value + ref[k].astype(F32)
        return value.astype(BF16)

    s_waits, f_waits = [], []

    @pl.when(second)
    def _():
        send(s_gb, s_cb, twin, 1)

    s_twin = len(sent) - 1

    @pl.when(first)
    def _():
        arrive(s_cb, s_twin)
        s_pb[...] = (s_gb[...].astype(F32) + s_cb[...].astype(F32)).astype(BF16)
        s_fb[f] = s_pb[f]
        s_waits.extend(scatter(s_pb, s_fb, f, to_f, f_ahead, f_behind, 0))

    finish(down_waits)
    zero_rim(take, 2)
    pool_grad = own_share
    for dx, dy in DIRS:
        pool_grad = pool_grad + take[1 - dx, 1 - dy].astype(F32)
    pool_grad = 0.125 * pool_grad
    high = pool_grad.astype(BF16)
    low = (pool_grad - high.astype(F32)).astype(BF16)
    spread = nt_dot(jnp.concatenate([high, low], axis=0), pairs)
    spread = spread[0:64] + spread[64:128]
    for a in range(2):
        for b in range(2):
            extd[a + 1, b + 1] = (spread * slope1[a, b]).astype(BF16)
    fd_waits = halo_start(extd)

    terms = jnp.zeros((192, 640), F32)
    for a in range(2):
        for b in range(2):
            own = extd[a + 1, b + 1]
            wide = own.astype(F32)
            lhs = jnp.concatenate(
                [shifted(wide, 1).astype(BF16), own, shifted(wide, -1).astype(BF16)], axis=0
            )
            terms = terms + nt_dot(lhs, stack(ext, a, b))

    per_peer = 16 // n_xy

    def put_fine(g, piece):
        for h in range(2):
            at = 2 * g + h
            row = 64 * (at % per_peer)
            f_gb[at // per_peer, row : row + 64] = piece[64 * h : 64 * h + 64]

        def part(buffer):
            if per_peer == 1:
                return buffer.at[2 * g : 2 * g + 2]
            return buffer.at[2 * g // per_peer, pl.ds(64 * (2 * g % per_peer), 128)]

        @pl.when(first)
        def _():
            send(part(f_gb), part(f_cb), twin, 0, lambda: part(f_gb))

        f_twin.append((len(sent) - 1, lambda: part(f_cb)))

    f_twin = []
    deal(terms, 8, 24, 8, put_fine)
    plane_waits, z_waits = [], []

    @pl.when(second)
    def _():
        finish(f_twin)
        f_pb[...] = (f_gb[...].astype(F32) + f_cb[...].astype(F32)).astype(BF16)
        f_xr[at_xy] = f_pb[at_xy]
        plane_waits.extend(
            scatter(f_pb, f_xr, at_xy, to_plane, plane_ahead, plane_behind, 1)
        )

    @pl.when(first)
    def _():
        finish(s_waits)
        s_zr[zh] = summed(s_fb, n_f)
        z_waits.extend(exchange(s_zr, zh, to_z, z_behind, 0))

    halo_finish(fd_waits)
    wb = w1b[...]
    for a in range(2):
        for b in range(2):
            rows = jnp.dot(wb, stack(extd, a, b), preferred_element_type=F32)
            plane = shifted(rows[0:64], 1) + rows[64:128] + shifted(rows[128:192], -1)
            for h in range(2):
                vrows[h, pl.ds(2 * a + b, 64, stride=4), :] = plane[:, 128 * h : 128 * h + 128]

    for c in range(64):
        for a in range(2):
            for h in range(2):
                vgrad_out[c, a, :, 128 * h : 128 * h + 128] = vrows[
                    h, 4 * c + 2 * a : 4 * c + 2 * a + 2
                ].astype(BF16)

    depth_waits, y_waits = [], []

    @pl.when(second)
    def _():
        finish(plane_waits)
        f_zr[at_z] = summed(f_xr, n_xy)
        depth_waits.extend(exchange(f_zr, at_z, to_depth, depth_behind, 1))

    @pl.when(first)
    def _():
        finish(z_waits)
        s_yr[y] = summed(s_zr, n_z)
        y_waits.extend(exchange(s_yr, y, to_y, y_behind, 0))

    finish(feat_waits)
    for k in range(n_f):
        crows[pl.ds(k, 16, stride=n_f), :] = featb[1, k].astype(F32)
    feat_out[...] = crows[...].reshape(16, 1, n_f, 128).astype(BF16)

    @pl.when(first)
    def _():
        finish(y_waits)
        s_os[...] = summed(s_yr, n_y)
        send(s_os, s_os, twin, 0)

    s_last = len(sent) - 1
    last_waits = []

    @pl.when(second)
    def _():
        finish(depth_waits)
        f_ag[at_xy] = summed(f_zr, 2 * n_z)
        waits = exchange(f_ag, at_xy, to_plane, plane_behind, 1)
        for slot, wait in zip([at_xy] + plane_behind, [None] + waits):
            if wait is not None:
                finish([wait])

            def part(slot=slot):
                return f_ag.at[slot]

            at = send(part(), part(), twin, 1, part)
            last_waits.append((at, part))
        arrive(s_os, s_last)

    @pl.when(first)
    def _():
        finish(last_waits)

    os_out[...] = s_os[...]
    ag_out[...] = f_ag[...]

    assert len(sent) <= N_SEMS
    drain(None)
    for d in DIRS:

        @pl.when(exists[d])
        def _(d=d):
            drain(d)

    @pl.when(first)
    def _():
        drain(0)

    @pl.when(second)
    def _():
        drain(1)


def unpack(n_f, scales, feat_in, vgrad_in, ag_in, os_in, feat_out, vgrad_out, g1_out, g2_out):
    fine_scale, bottom_scale = scales
    feat_out[...] = feat_in[...]
    vgrad_out[...] = vgrad_in[...]
    for k in range(15):
        dz, c = k // 5, k % 5
        tile = os_in[16 * k : 16 * k + 16].astype(F32) * bottom_scale
        g2_out[6 * c + dz] = tile[:, 0:64]
        if c < 4:
            g2_out[6 * c + 3 + dz] = pltpu.roll(tile, 64, 1)[:, 0:64]
    for g in range(n_f):
        per_peer = 16 // ag_in.shape[0]
        both = []
        for at in (2 * g, 2 * g + 1):
            start = 64 * (at % per_peer)
            both.append(ag_in[at // per_peer, start : start + 64].astype(F32) * fine_scale)
        for k in range(15):
            row = 24 * g + 8 * (k // 5)
            dz, o = row // 64, row % 64
            c = k % 5
            tile = both[k // 8][8 * (k % 8) : 8 * (k % 8) + 8]
            g1_out[6 * c + dz, o : o + 8] = tile[:, 0:64]
            if c < 4:
                g1_out[6 * c + 3 + dz, o : o + 8] = pltpu.roll(tile, 64, 1)[:, 0:64]


def local(sizes, volume, first_weight, second_weight, cotangent):
    n_s, n_f, n_y, n_z = sizes
    n_xy = n_f // 2 * n_y
    scales = (
        1.0 / float(n_s * 2 * n_f * 2 * 256) ** 0.5,
        1.0 / float(n_s * n_f * 128) ** 0.5,
    )
    vmem = pl.BlockSpec(memory_space=pltpu.VMEM)
    whole = pl.BlockSpec(memory_space=pltpu.HBM)
    operands = (volume, cotangent, first_weight, second_weight)
    shape = jax.ShapeDtypeStruct
    features, volume_grad, fine, bottom = pl.pallas_call(
        functools.partial(kernel, sizes),
        out_shape=(
            shape((16, 1, n_f, 128), BF16),
            shape((64, 2, 2, 256), BF16),
            shape((n_xy, 1024 // n_xy, 128), BF16),
            shape((256, 128), BF16),
        ),
        in_specs=[whole] * 4,
        out_specs=(vmem,) * 4,
        scratch_shapes=[
            pltpu.VMEM((64, 2, 2, 256), BF16),
            pltpu.VMEM((16, 1, n_f, 128), BF16),
            pltpu.VMEM((27, 64, 64), BF16),
            pltpu.VMEM((27, 16, 64), BF16),
            pltpu.VMEM((2, 256, 128), F32),
            pltpu.VMEM((16 * n_f, 128), F32),
            pltpu.VMEM((n_f, 16, 128), BF16),
            pltpu.VMEM((192, 640), BF16),
            pltpu.VMEM((192, 640), BF16),
            pltpu.VMEM((16, 16, 128), BF16),
            pltpu.VMEM((4, 4, 64, 256), BF16),
            pltpu.VMEM((4, 4, 64, 256), BF16),
            pltpu.VMEM((2, 2, 64, 256), F32),
            pltpu.VMEM((n_f, 16, 128), BF16),
            pltpu.VMEM((2, n_f, 8, 16, 128), BF16),
            pltpu.VMEM((3, 640, 128), BF16),
            pltpu.VMEM((4, 3, 64, 128), BF16),
            pltpu.VMEM((9, 64, 128), BF16),
            pltpu.VMEM((3, 3, 64, 128), BF16),
            pltpu.VMEM((2, n_f, 16, 128), BF16),
            pltpu.VMEM((n_f, 256, 128), BF16),
            pltpu.VMEM((n_f, 256, 128), BF16),
            pltpu.VMEM((n_f, 256, 128), BF16),
            pltpu.VMEM((n_f, 256, 128), BF16),
            pltpu.VMEM((n_y, 256, 128), BF16),
            pltpu.VMEM((n_z, 256, 128), BF16),
            pltpu.VMEM((256, 128), BF16),
            pltpu.VMEM((n_xy, 1024 // n_xy, 128), BF16),
            pltpu.VMEM((n_xy, 1024 // n_xy, 128), BF16),
            pltpu.VMEM((n_xy, 1024 // n_xy, 128), BF16),
            pltpu.VMEM((n_xy, 1024 // n_xy, 128), BF16),
            pltpu.VMEM((2 * n_z, 1024 // n_xy, 128), BF16),
            pltpu.VMEM((n_xy, 1024 // n_xy, 128), BF16),
            pltpu.SemaphoreType.DMA((4,)),
            pltpu.SemaphoreType.DMA((N_SEMS,)),
            pltpu.SemaphoreType.DMA((N_SEMS,)),
        ],
        compiler_params=pltpu.CompilerParams(
            collective_id=0, has_side_effects=True, vmem_limit_bytes=24 * 1024 * 1024
        ),
        name="block",
    )(*(pltpu.with_memory_space_constraint(v, pltpu.HBM) for v in operands))
    return pl.pallas_call(
        functools.partial(unpack, n_f, scales),
        out_shape=(
            shape((16, 1, n_f, 128), BF16),
            shape((64, 2, 2, 256), BF16),
            shape((27, 64, 64), F32),
            shape((27, 16, 64), F32),
        ),
        in_specs=[vmem] * 4,
        out_specs=(vmem,) * 4,
        compiler_params=pltpu.CompilerParams(vmem_limit_bytes=24 * 1024 * 1024),
        name="unpack",
    )(features, volume_grad, fine, bottom)


def solution(mesh):
    n_s, n_f = mesh.shape["space"], mesh.shape["filt"]
    n_z = 4 if n_s % 8 == 0 else 1
    sizes = (n_s, n_f, n_s // (2 * n_z), n_z)
    placed = (
        P(None, "space", "filt", None),
        P(),
        P(None, "filt", None),
        P("filt", "space", None, None),
    )
    return jax.shard_map(
        functools.partial(local, sizes),
        mesh=mesh,
        in_specs=placed,
        out_specs=(
            P("filt", "space", None, None),
            P(None, "space", "filt", None),
            P(),
            P(None, "filt", None),
        ),
        check_vma=False,
    )
```

```python
import functools

import jax
import jax.numpy as jnp
from jax import lax
from jax.experimental import pallas as pl
from jax.experimental.pallas import tpu as pltpu
from jax.sharding import PartitionSpec as P

MESH = pl.DeviceIdType.MESH
F32 = jnp.float32
BF16 = jnp.bfloat16
DIRS = [(-1, -1), (-1, 1), (1, -1), (1, 1), (-1, 0), (1, 0), (0, -1), (0, 1)]
N_SEMS = 34


def sigmoid(v):
    return 1.0 / (1.0 + jnp.exp(-v))


def shifted(values, by):
    if by == 0:
        return values
    length = values.shape[1]
    lane = lax.broadcasted_iota(jnp.int32, values.shape, 1)
    if by == 1:
        return jnp.where(lane == length - 1, 0.0, pltpu.roll(values, length - 1, 1))
    return jnp.where(lane == 0, 0.0, pltpu.roll(values, 1, 1))


def nt_dot(a, b):
    return lax.dot_general(a, b, (((1,), (1,)), ((), ())), preferred_element_type=F32)


def side_by_side(left, right):
    return jnp.concatenate([left, right], axis=1)


def kernel(
    sizes,
    vol_hbm,
    cot_hbm,
    w1_hbm,
    w2_hbm,
    feat_out,
    vgrad_out,
    ag_out,
    os_out,
    vraw,
    craw,
    w1raw,
    w2raw,
    vrows,
    crows,
    cotb,
    w1f,
    w1b,
    w2p,
    ext,
    extd,
    slope1,
    cotg,
    w2g,
    w2t,
    ps,
    give,
    take,
    featb,
    s_gb,
    s_cb,
    s_pb,
    s_fb,
    s_yr,
    s_zr,
    s_os,
    f_gb,
    f_cb,
    f_pb,
    f_xr,
    f_zr,
    f_ag,
    load_sem,
    send_sem,
    recv_sem,
):
    n_s, n_f, n_y, n_z = sizes
    s = lax.axis_index("space")
    f = lax.axis_index("filt")
    core = lax.rem(s, 2)
    zh = lax.rem(s // 2, n_z)
    y = s // (2 * n_z)

    loads = []
    for at, (whole, raw) in enumerate(
        ((vol_hbm, vraw), (w2_hbm, w2raw), (cot_hbm, craw), (w1_hbm, w1raw))
    ):
        load = pltpu.make_async_copy(whole, raw, load_sem.at[at])
        load.start()
        loads.append(load)

    def near(dx, dy):
        return (lax.rem(s + dx + n_s, n_s), lax.rem(f + dy + n_f, n_f))

    def along_f(j):
        return (s, lax.rem(f + j, n_f))

    def along_y(j):
        return ((lax.rem(y + j, n_y) * n_z + zh) * 2 + core, f)

    def along_z(j):
        return ((y * n_z + lax.rem(zh + j, n_z)) * 2 + core, f)

    twin = (s + 1 - 2 * core, f)
    n_x = n_f // 2
    n_xy = n_x * n_y
    x, zl = lax.rem(f, n_x), f // n_x
    at_xy = y * n_x + x
    at_z = 2 * zh + zl

    def over_plane(j):
        to = lax.rem(at_xy + j, n_xy)
        return ((to // n_x * n_z + zh) * 2 + core, zl * n_x + lax.rem(to, n_x))

    def over_depth(j):
        to = lax.rem(at_z + j, 2 * n_z)
        return ((y * n_z + to // 2) * 2 + core, lax.rem(to, 2) * n_x + x)

    to_f = [along_f(j) for j in range(1, n_f)]
    to_y = [along_y(j) for j in range(1, n_y)]
    to_z = [along_z(j) for j in range(1, n_z)]
    to_plane = [over_plane(j) for j in range(1, n_xy)]
    to_depth = [over_depth(j) for j in range(1, 2 * n_z)]

    def ahead(me, count):
        return [lax.rem(me + j, count) for j in range(1, count)]

    f_ahead = ahead(f, n_f)
    plane_ahead = ahead(at_xy, n_xy)
    first, second = core == 0, core == 1
    in_s = {-1: s > 0, 0: s >= 0, 1: s < n_s - 1}
    in_f = {-1: f > 0, 0: f >= 0, 1: f < n_f - 1}
    exists = {(dx, dy): in_s[dx] & in_f[dy] for dx, dy in DIRS}
    beside = {d: near(*d) for d in DIRS}
    flip = (1 - zl) * n_x + x
    x_ahead = [zl * n_x + lax.rem(x + j, n_x) for j in range(1, n_x)]

    peers = [beside[d] for d in DIRS] + to_f + to_plane + to_depth
    barrier = pltpu.get_barrier_semaphore()
    for peer in peers:
        pl.semaphore_signal(barrier, inc=1, device_id=peer, device_id_type=MESH)

    loads[0].wait()
    for c in range(64):
        for a in range(2):
            for h in range(2):
                vrows[h, 4 * c + 2 * a : 4 * c + 2 * a + 2] = vraw[
                    c, a, :, 128 * h : 128 * h + 128
                ].astype(F32)
    for a in range(2):
        for b in range(2):
            for h in range(2):
                ext[a + 1, b + 1, :, 128 * h : 128 * h + 128] = vrows[
                    h, pl.ds(2 * a + b, 64, stride=4), :
                ].astype(BF16)
    pl.semaphore_wait(barrier, len(peers))

    used = []
    owed = {}

    def fresh(only, size):
        at = len(used)
        used.append(at)
        owed.setdefault(only, []).append((at, size))
        return at

    def send(src, dst, device, at):
        pltpu.make_async_remote_copy(
            src_ref=src,
            dst_ref=dst,
            send_sem=send_sem.at[at],
            recv_sem=recv_sem.at[at],
            device_id=device,
            device_id_type=MESH,
        ).start()

    def arrive(ref, at):
        ref = ref() if callable(ref) else ref
        pltpu.make_async_copy(ref, ref, recv_sem.at[at]).wait()

    def drain(only):
        for at, size in owed[only]:
            ref = size()
            pltpu.make_async_copy(ref, ref, send_sem.at[at]).wait()

    def src_part(d):
        return {1: 2, -1: 1, 0: slice(1, 3)}[d]

    def dst_part(d):
        return {1: 0, -1: 3, 0: slice(1, 3)}[d]

    def halo_start(field):
        out = []
        for d in DIRS:
            dx, dy = d

            def source(dx=dx, dy=dy):
                return field.at[src_part(dx), src_part(dy)]

            def target(dx=dx, dy=dy):
                return field.at[dst_part(dx), dst_part(dy)]

            at = fresh(d, source)

            @pl.when(exists[d])
            def _(d=d, source=source, target=target, at=at):
                send(source(), target(), beside[d], at)

            out.append((d, at, target))
        return out

    def halo_finish(waits):
        for (dx, dy), at, target in waits:

            @pl.when(exists[-dx, -dy])
            def _(at=at, target=target):
                arrive(target, at)

    def zero_rim(field, last):
        @pl.when(s == 0)
        def _():
            for b in range(last + 1):
                field[0, b] = jnp.zeros(field.shape[2:], field.dtype)

        @pl.when(s == n_s - 1)
        def _():
            for b in range(last + 1):
                field[last, b] = jnp.zeros(field.shape[2:], field.dtype)

        @pl.when(f == 0)
        def _():
            for a in range(last + 1):
                field[a, 0] = jnp.zeros(field.shape[2:], field.dtype)

        @pl.when(f == n_f - 1)
        def _():
            for a in range(last + 1):
                field[a, last] = jnp.zeros(field.shape[2:], field.dtype)

    vol_waits = halo_start(ext)
    zero_rim(ext, 3)
    zero_rim(extd, 3)

    loads[1].wait()
    for k in range(15):
        dz, c = k // 5, k % 5
        right = w2raw[6 * c + 3 + dz] if c < 4 else jnp.zeros((16, 64), BF16)
        w2p[k] = side_by_side(w2raw[6 * c + dz], right)
    w2p[15] = jnp.zeros((16, 128), BF16)
    half = w2p.at[pl.ds(8 * core, 8)]
    w2_flip, w2_row = fresh(None, lambda: half), fresh(None, lambda: w2g.at[core, 0 : n_x - 1])
    send(half, w2g.at[core, f], (s, flip), w2_flip)
    for to in x_ahead:
        send(half, w2g.at[core, f], (s, to), w2_row)
    w2g[core, f] = w2p[pl.ds(8 * core, 8)]

    loads[2].wait()
    crows[...] = craw[...].reshape(16 * n_f, 128).astype(F32)
    for k in range(n_f):
        cotb[k] = crows[pl.ds(k, 16, stride=n_f), :].astype(BF16)
    cot_at = fresh(None, lambda: cotb.at[0 : n_f - 1])
    for other, peer in zip(f_ahead, to_f):
        send(cotb.at[other], cotg.at[f], peer, cot_at)
    cotg[f] = cotb[f]

    loads[3].wait()
    for k in range(15):
        dz, c = k // 5, k % 5
        rows = slice(64 * dz, 64 * dz + 64)
        cols = slice(128 * c, 128 * c + 128)
        right = w1raw[6 * c + 3 + dz] if c < 4 else jnp.zeros((64, 64), BF16)
        w1f[rows, cols] = side_by_side(w1raw[6 * c + dz], right)
        back = [w1raw[3 * (8 - 2 * c) + dz]]
        back.append(w1raw[3 * (7 - 2 * c) + dz] if c < 4 else jnp.zeros((64, 64), BF16))
        w1b[rows, cols] = jnp.concatenate(back, axis=0).astype(F32).T.astype(BF16)
    ps[3, 0] = jnp.zeros((64, 128), BF16)
    pair_row = lax.broadcasted_iota(jnp.int32, (256, 128), 0)
    pair_col = lax.broadcasted_iota(jnp.int32, (256, 128), 1)
    below = pair_row - 2 * pair_col
    pairs = jnp.where((below == 0) | (below == 1), 1.0, 0.0).astype(BF16)

    def stack(field, a, b):
        planes = [field[a + i, b + j] for i in range(3) for j in range(3)]
        return jnp.concatenate(planes + [jnp.zeros((64, 256), BF16)], axis=0)

    arrive(w2g.at[core, flip], w2_flip)
    w2_pass = fresh(None, lambda: w2g.at[core, 0 : n_x - 1])
    for to in x_ahead:
        send(w2g.at[core, flip], w2g.at[core, flip], (s, to), w2_pass)
    halo_finish(vol_waits)

    wf = w1f[...]
    total = jnp.zeros((64, 128), F32)
    for a in range(2):
        for b in range(2):
            rows = jnp.dot(wf, stack(ext, a, b), preferred_element_type=F32)
            pre = shifted(rows[0:64], -1) + rows[64:128] + shifted(rows[128:192], 1)
            gate = sigmoid(pre)
            slope1[a, b] = gate * (1.0 + pre * (1.0 - gate))
            hidden = (pre * gate).astype(BF16)
            total = total + jnp.dot(hidden, pairs, preferred_element_type=F32)
    ps[1, 1] = (0.125 * total).astype(BF16)

    pool_at = fresh(None, lambda: ps.at[0:4, 0:2])
    for d in DIRS:
        send(ps.at[1, 1], ps.at[1 - d[0], 1 - d[1]], beside[d], pool_at)

    arrive(lambda: w2g.at[core, 0 : n_x - 1], w2_row)
    arrive(lambda: w2g.at[core, 0 : n_x - 1], w2_pass)
    w2_twin = fresh(None, lambda: w2g.at[core])
    send(w2g.at[core], w2g.at[core], twin, w2_twin)
    arrive(lambda: cotg.at[0 : n_f - 1], cot_at)
    arrive(lambda: w2g.at[1 - core], w2_twin)
    w2 = []
    for dz in range(3):
        tiles = [
            w2g[k // 8, :, k % 8].reshape(16 * n_f, 128) for k in range(5 * dz, 5 * dz + 5)
        ]
        w2.append(jnp.concatenate(tiles, axis=1))
        for c in range(5):
            w2t[dz, 128 * c : 128 * c + 128] = tiles[c].astype(F32).T.astype(BF16)

    arrive(lambda: ps.at[0:4, 0:2], pool_at)
    zero_rim(ps, 2)

    around = jnp.concatenate(
        [ps[i, j] for i in range(3) for j in range(3)] + [ps[3, 0]], axis=0
    )
    rows = [jnp.dot(w, around, preferred_element_type=F32) for w in w2]
    pre = shifted(rows[0], -1) + rows[1] + shifted(rows[2], 1)
    gate = sigmoid(pre)
    down = cotg[...].reshape(128, 128).astype(F32) * (gate * (1.0 + pre * (1.0 - gate)))
    down_own = down.astype(BF16)

    rows = [jnp.dot(w2t[dz], down_own, preferred_element_type=F32) for dz in range(3)]
    share = shifted(rows[0], 1) + rows[1] + shifted(rows[2], -1)
    down_at = fresh(None, lambda: give.at[0:8])
    for dx, dy in DIRS:
        slot = 3 * (dx + 1) + dy + 1
        give[slot] = share[64 * slot : 64 * slot + 64].astype(BF16)
        send(give.at[slot], take.at[1 - dx, 1 - dy], beside[dx, dy], down_at)
    own_share = share[256:320]
    featb[0] = (pre * gate).astype(BF16).reshape(n_f, 16, 128)

    feat_at = fresh(None, lambda: featb.at[0, 0 : n_f - 1])
    for other, peer in zip(f_ahead, to_f):
        send(featb.at[0, other], featb.at[1, f], peer, feat_at)
    featb[1, f] = featb[0, f]

    lhs = jnp.concatenate(
        [shifted(down, 1).astype(BF16), down_own, shifted(down, -1).astype(BF16)], axis=0
    )
    terms = nt_dot(lhs, around)

    def deal(values, height, per, step, put):
        for g in range(n_f):
            tiles = [
                values[per * g + step * r : per * g + step * r + height, 128 * c : 128 * c + 128]
                for r in range(3)
                for c in range(5)
            ]
            tiles.append(jnp.zeros((height, 128), F32))
            put(g, jnp.concatenate(tiles, axis=0).astype(BF16))

    def put_bottom(g, piece):
        s_gb[g] = piece

    deal(terms, 16, 16, 128, put_bottom)

    def exchange(ref, mine, peers, only):
        at = fresh(only, lambda: ref.at[0 : len(peers)])
        for peer in peers:
            send(ref.at[mine], ref.at[mine], peer, at)
        return at, lambda: ref.at[0 : len(peers)]

    def scatter(out, into, mine, peers, theirs, only):
        at = fresh(only, lambda: out.at[0 : len(peers)])
        for peer, other in zip(peers, theirs):
            send(out.at[other], into.at[mine], peer, at)
        return at, lambda: into.at[0 : len(peers)]

    def finish(waits):
        for at, ref in waits:
            arrive(ref, at)

    def summed(ref, count):
        value = ref[0].astype(F32)
        for k in range(1, count):
            value = value + ref[k].astype(F32)
        return value.astype(BF16)

    s_waits = []
    s_twin = fresh(1, lambda: s_gb)

    @pl.when(second)
    def _():
        send(s_gb, s_cb, twin, s_twin)

    @pl.when(first)
    def _():
        arrive(s_cb, s_twin)
        s_pb[...] = (s_gb[...].astype(F32) + s_cb[...].astype(F32)).astype(BF16)
        s_fb[f] = s_pb[f]
        s_waits.append(scatter(s_pb, s_fb, f, to_f, f_ahead, 0))

    arrive(lambda: give.at[0:8], down_at)
    zero_rim(take, 2)
    pool_grad = own_share
    for dx, dy in DIRS:
        pool_grad = pool_grad + take[1 - dx, 1 - dy].astype(F32)
    pool_grad = 0.125 * pool_grad
    high = pool_grad.astype(BF16)
    low = (pool_grad - high.astype(F32)).astype(BF16)
    spread = nt_dot(jnp.concatenate([high, low], axis=0), pairs)
    spread = spread[0:64] + spread[64:128]
    for a in range(2):
        for b in range(2):
            extd[a + 1, b + 1] = (spread * slope1[a, b]).astype(BF16)

    terms = jnp.zeros((192, 640), F32)
    for a in range(2):
        for b in range(2):
            own = extd[a + 1, b + 1]
            wide = own.astype(F32)
            lhs = jnp.concatenate(
                [shifted(wide, 1).astype(BF16), own, shifted(wide, -1).astype(BF16)], axis=0
            )
            terms = terms + nt_dot(lhs, stack(ext, a, b))

    per_peer = 16 // n_xy

    def put_fine(g, piece):
        for h in range(2):
            at = 2 * g + h
            row = 64 * (at % per_peer)
            f_gb[at // per_peer, row : row + 64] = piece[64 * h : 64 * h + 64]

        def part(buffer):
            if per_peer == 1:
                return buffer.at[2 * g : 2 * g + 2]
            return buffer.at[2 * g // per_peer, pl.ds(64 * (2 * g % per_peer), 128)]

        @pl.when(first)
        def _():
            send(part(f_gb), part(f_cb), twin, f_twin)

    f_twin = fresh(0, lambda: f_gb)
    deal(terms, 8, 24, 8, put_fine)
    plane_waits, z_waits = [], []

    @pl.when(second)
    def _():
        arrive(f_cb, f_twin)
        f_pb[...] = (f_gb[...].astype(F32) + f_cb[...].astype(F32)).astype(BF16)
        f_xr[at_xy] = f_pb[at_xy]
        plane_waits.append(scatter(f_pb, f_xr, at_xy, to_plane, plane_ahead, 1))

    fd_waits = halo_start(extd)

    @pl.when(first)
    def _():
        finish(s_waits)
        s_zr[zh] = summed(s_fb, n_f)
        z_waits.append(exchange(s_zr, zh, to_z, 0))

    halo_finish(fd_waits)
    wb = w1b[...]
    for a in range(2):
        for b in range(2):
            rows = jnp.dot(wb, stack(extd, a, b), preferred_element_type=F32)
            plane = shifted(rows[0:64], 1) + rows[64:128] + shifted(rows[128:192], -1)
            for h in range(2):
                vrows[h, pl.ds(2 * a + b, 64, stride=4), :] = plane[:, 128 * h : 128 * h + 128]

    for c in range(64):
        for a in range(2):
            for h in range(2):
                vgrad_out[c, a, :, 128 * h : 128 * h + 128] = vrows[
                    h, 4 * c + 2 * a : 4 * c + 2 * a + 2
                ].astype(BF16)

    depth_waits, y_waits = [], []

    @pl.when(second)
    def _():
        finish(plane_waits)
        f_zr[at_z] = summed(f_xr, n_xy)
        depth_waits.append(exchange(f_zr, at_z, to_depth, 1))

    @pl.when(first)
    def _():
        finish(z_waits)
        s_yr[y] = summed(s_zr, n_z)
        y_waits.append(exchange(s_yr, y, to_y, 0))

    arrive(lambda: featb.at[1, 0 : n_f - 1], feat_at)
    for k in range(n_f):
        crows[pl.ds(k, 16, stride=n_f), :] = featb[1, k].astype(F32)
    feat_out[...] = crows[...].reshape(16, 1, n_f, 128).astype(BF16)

    s_last, f_last = fresh(0, lambda: s_os), fresh(1, lambda: f_ag)

    @pl.when(first)
    def _():
        finish(y_waits)
        s_os[...] = summed(s_yr, n_y)
        send(s_os, s_os, twin, s_last)

    @pl.when(second)
    def _():
        finish(depth_waits)
        f_ag[at_xy] = summed(f_zr, 2 * n_z)
        finish([exchange(f_ag, at_xy, to_plane, 1)])
        send(f_ag, f_ag, twin, f_last)
        arrive(s_os, s_last)

    @pl.when(first)
    def _():
        arrive(f_ag, f_last)

    os_out[...] = s_os[...]
    ag_out[...] = f_ag[...]

    assert len(used) <= N_SEMS
    drain(None)
    for d in DIRS:

        @pl.when(exists[d])
        def _(d=d):
            drain(d)

    @pl.when(first)
    def _():
        drain(0)

    @pl.when(second)
    def _():
        drain(1)


def unpack(n_f, scales, feat_in, vgrad_in, ag_in, os_in, feat_out, vgrad_out, g1_out, g2_out):
    fine_scale, bottom_scale = scales
    feat_out[...] = feat_in[...]
    vgrad_out[...] = vgrad_in[...]
    for k in range(15):
        dz, c = k // 5, k % 5
        tile = os_in[16 * k : 16 * k + 16].astype(F32) * bottom_scale
        g2_out[6 * c + dz] = tile[:, 0:64]
        if c < 4:
            g2_out[6 * c + 3 + dz] = pltpu.roll(tile, 64, 1)[:, 0:64]
    for g in range(n_f):
        per_peer = 16 // ag_in.shape[0]
        both = []
        for at in (2 * g, 2 * g + 1):
            start = 64 * (at % per_peer)
            both.append(ag_in[at // per_peer, start : start + 64].astype(F32) * fine_scale)
        for k in range(15):
            row = 24 * g + 8 * (k // 5)
            dz, o = row // 64, row % 64
            c = k % 5
            tile = both[k // 8][8 * (k % 8) : 8 * (k % 8) + 8]
            g1_out[6 * c + dz, o : o + 8] = tile[:, 0:64]
            if c < 4:
                g1_out[6 * c + 3 + dz, o : o + 8] = pltpu.roll(tile, 64, 1)[:, 0:64]


def local(sizes, volume, first_weight, second_weight, cotangent):
    n_s, n_f, n_y, n_z = sizes
    n_xy = n_f // 2 * n_y
    scales = (
        1.0 / float(n_s * 2 * n_f * 2 * 256) ** 0.5,
        1.0 / float(n_s * n_f * 128) ** 0.5,
    )
    vmem = pl.BlockSpec(memory_space=pltpu.VMEM)
    whole = pl.BlockSpec(memory_space=pltpu.HBM)
    operands = (volume, cotangent, first_weight, second_weight)
    shape = jax.ShapeDtypeStruct
    features, volume_grad, fine, bottom = pl.pallas_call(
        functools.partial(kernel, sizes),
        out_shape=(
            shape((16, 1, n_f, 128), BF16),
            shape((64, 2, 2, 256), BF16),
            shape((n_xy, 1024 // n_xy, 128), BF16),
            shape((256, 128), BF16),
        ),
        in_specs=[whole] * 4,
        out_specs=(vmem,) * 4,
        scratch_shapes=[
            pltpu.VMEM((64, 2, 2, 256), BF16),
            pltpu.VMEM((16, 1, n_f, 128), BF16),
            pltpu.VMEM((27, 64, 64), BF16),
            pltpu.VMEM((27, 16, 64), BF16),
            pltpu.VMEM((2, 256, 128), F32),
            pltpu.VMEM((16 * n_f, 128), F32),
            pltpu.VMEM((n_f, 16, 128), BF16),
            pltpu.VMEM((192, 640), BF16),
            pltpu.VMEM((192, 640), BF16),
            pltpu.VMEM((16, 16, 128), BF16),
            pltpu.VMEM((4, 4, 64, 256), BF16),
            pltpu.VMEM((4, 4, 64, 256), BF16),
            pltpu.VMEM((2, 2, 64, 256), F32),
            pltpu.VMEM((n_f, 16, 128), BF16),
            pltpu.VMEM((2, n_f, 8, 16, 128), BF16),
            pltpu.VMEM((3, 640, 128), BF16),
            pltpu.VMEM((4, 3, 64, 128), BF16),
            pltpu.VMEM((9, 64, 128), BF16),
            pltpu.VMEM((3, 3, 64, 128), BF16),
            pltpu.VMEM((2, n_f, 16, 128), BF16),
            pltpu.VMEM((n_f, 256, 128), BF16),
            pltpu.VMEM((n_f, 256, 128), BF16),
            pltpu.VMEM((n_f, 256, 128), BF16),
            pltpu.VMEM((n_f, 256, 128), BF16),
            pltpu.VMEM((n_y, 256, 128), BF16),
            pltpu.VMEM((n_z, 256, 128), BF16),
            pltpu.VMEM((256, 128), BF16),
            pltpu.VMEM((n_xy, 1024 // n_xy, 128), BF16),
            pltpu.VMEM((n_xy, 1024 // n_xy, 128), BF16),
            pltpu.VMEM((n_xy, 1024 // n_xy, 128), BF16),
            pltpu.VMEM((n_xy, 1024 // n_xy, 128), BF16),
            pltpu.VMEM((2 * n_z, 1024 // n_xy, 128), BF16),
            pltpu.VMEM((n_xy, 1024 // n_xy, 128), BF16),
            pltpu.SemaphoreType.DMA((4,)),
            pltpu.SemaphoreType.DMA((N_SEMS,)),
            pltpu.SemaphoreType.DMA((N_SEMS,)),
        ],
        compiler_params=pltpu.CompilerParams(
            collective_id=0, has_side_effects=True, vmem_limit_bytes=24 * 1024 * 1024
        ),
        name="block",
    )(*(pltpu.with_memory_space_constraint(v, pltpu.HBM) for v in operands))
    return pl.pallas_call(
        functools.partial(unpack, n_f, scales),
        out_shape=(
            shape((16, 1, n_f, 128), BF16),
            shape((64, 2, 2, 256), BF16),
            shape((27, 64, 64), F32),
            shape((27, 16, 64), F32),
        ),
        in_specs=[vmem] * 4,
        out_specs=(vmem,) * 4,
        compiler_params=pltpu.CompilerParams(vmem_limit_bytes=24 * 1024 * 1024),
        name="unpack",
    )(features, volume_grad, fine, bottom)


def solution(mesh):
    n_s, n_f = mesh.shape["space"], mesh.shape["filt"]
    n_z = 4 if n_s % 8 == 0 else 1
    sizes = (n_s, n_f, n_s // (2 * n_z), n_z)
    placed = (
        P(None, "space", "filt", None),
        P(),
        P(None, "filt", None),
        P("filt", "space", None, None),
    )
    return jax.shard_map(
        functools.partial(local, sizes),
        mesh=mesh,
        in_specs=placed,
        out_specs=(
            P("filt", "space", None, None),
            P(None, "space", "filt", None),
            P(),
            P(None, "filt", None),
        ),
        check_vma=False,
    )
```

```python
import functools

import jax
import jax.numpy as jnp
from jax import lax
from jax.experimental import pallas as pl
from jax.experimental.pallas import tpu as pltpu
from jax.sharding import PartitionSpec as P

MESH = pl.DeviceIdType.MESH
F32 = jnp.float32
BF16 = jnp.bfloat16
DIRS = [(-1, -1), (-1, 1), (1, -1), (1, 1), (-1, 0), (1, 0), (0, -1), (0, 1)]
N_SEMS = 34


def far_first(*rings):
    offsets = [()]
    for length in rings:
        offsets = [o + (k,) for o in offsets for k in range(length)]
    hops = [sum(min(k, n - k) for k, n in zip(o, rings)) for o in offsets]
    order = sorted(range(1, len(offsets)), key=lambda i: -hops[i])
    return [offsets[i] for i in order]


def sigmoid(v):
    return 1.0 / (1.0 + jnp.exp(-v))


def shifted(values, by):
    if by == 0:
        return values
    length = values.shape[1]
    lane = lax.broadcasted_iota(jnp.int32, values.shape, 1)
    if by == 1:
        return jnp.where(lane == length - 1, 0.0, pltpu.roll(values, length - 1, 1))
    return jnp.where(lane == 0, 0.0, pltpu.roll(values, 1, 1))


def nt_dot(a, b):
    return lax.dot_general(a, b, (((1,), (1,)), ((), ())), preferred_element_type=F32)


def side_by_side(left, right):
    return jnp.concatenate([left, right], axis=1)


def kernel(
    sizes,
    vol_hbm,
    cot_hbm,
    w1_hbm,
    w2_hbm,
    feat_out,
    vgrad_out,
    ag_out,
    os_out,
    vraw,
    craw,
    w1raw,
    w2raw,
    vrows,
    crows,
    cotb,
    w1f,
    w1b,
    w2p,
    ext,
    extd,
    slope1,
    cotg,
    w2g,
    w2t,
    ps,
    give,
    take,
    featb,
    s_gb,
    s_cb,
    s_pb,
    s_fb,
    s_yr,
    s_zr,
    s_os,
    f_gb,
    f_cb,
    f_pb,
    f_xr,
    f_zr,
    f_ag,
    load_sem,
    send_sem,
    recv_sem,
):
    n_s, n_f, n_y, n_z = sizes
    s = lax.axis_index("space")
    f = lax.axis_index("filt")
    core = lax.rem(s, 2)
    zh = lax.rem(s // 2, n_z)
    y = s // (2 * n_z)

    loads = []
    for at, (whole, raw) in enumerate(
        ((vol_hbm, vraw), (w2_hbm, w2raw), (cot_hbm, craw), (w1_hbm, w1raw))
    ):
        load = pltpu.make_async_copy(whole, raw, load_sem.at[at])
        load.start()
        loads.append(load)

    def near(dx, dy):
        return (lax.rem(s + dx + n_s, n_s), lax.rem(f + dy + n_f, n_f))

    twin = (s + 1 - 2 * core, f)
    n_x = n_f // 2
    n_xy = n_x * n_y
    x, zl = lax.rem(f, n_x), f // n_x
    at_xy = y * n_x + x
    at_z = 2 * zh + zl

    def device(y_to, zh_to, zl_to, x_to):
        return ((y_to * n_z + zh_to) * 2 + core, zl_to * n_x + x_to)

    def turned_by(position, by, length):
        return position if by == 0 else lax.rem(position + by, length)

    to_f, f_ahead = [], []
    for p, q in far_first(2, n_x):
        to_f.append(device(y, zh, turned_by(zl, p, 2), turned_by(x, q, n_x)))
        f_ahead.append(to_f[-1][1])
    to_y = [device(turned_by(y, p, n_y), zh, zl, x) for (p,) in far_first(n_y)]
    to_z = [device(y, turned_by(zh, p, n_z), zl, x) for (p,) in far_first(n_z)]
    to_plane, plane_ahead = [], []
    for p, q in far_first(n_y, n_x):
        y_to, x_to = turned_by(y, p, n_y), turned_by(x, q, n_x)
        to_plane.append(device(y_to, zh, zl, x_to))
        plane_ahead.append(y_to * n_x + x_to)
    to_depth = []
    for (p,) in far_first(2 * n_z):
        to = turned_by(at_z, p, 2 * n_z)
        to_depth.append(device(y, to // 2, lax.rem(to, 2), x))
    first, second = core == 0, core == 1
    in_s = {-1: s > 0, 0: s >= 0, 1: s < n_s - 1}
    in_f = {-1: f > 0, 0: f >= 0, 1: f < n_f - 1}
    exists = {(dx, dy): in_s[dx] & in_f[dy] for dx, dy in DIRS}
    beside = {d: near(*d) for d in DIRS}
    flip = (1 - zl) * n_x + x
    x_ahead = [zl * n_x + lax.rem(x + j, n_x) for j in range(1, n_x)]

    peers = [beside[d] for d in DIRS] + to_f + to_plane + to_depth
    barrier = pltpu.get_barrier_semaphore()
    for peer in peers:
        pl.semaphore_signal(barrier, inc=1, device_id=peer, device_id_type=MESH)

    loads[0].wait()
    for c in range(64):
        for a in range(2):
            for h in range(2):
                vrows[h, 4 * c + 2 * a : 4 * c + 2 * a + 2] = vraw[
                    c, a, :, 128 * h : 128 * h + 128
                ].astype(F32)
    for a in range(2):
        for b in range(2):
            for h in range(2):
                ext[a + 1, b + 1, :, 128 * h : 128 * h + 128] = vrows[
                    h, pl.ds(2 * a + b, 64, stride=4), :
                ].astype(BF16)
    pl.semaphore_wait(barrier, len(peers))

    used = []
    owed = {}

    def fresh(only, size):
        at = len(used)
        used.append(at)
        owed.setdefault(only, []).append((at, size))
        return at

    def send(src, dst, device, at):
        pltpu.make_async_remote_copy(
            src_ref=src,
            dst_ref=dst,
            send_sem=send_sem.at[at],
            recv_sem=recv_sem.at[at],
            device_id=device,
            device_id_type=MESH,
        ).start()

    def arrive(ref, at):
        ref = ref() if callable(ref) else ref
        pltpu.make_async_copy(ref, ref, recv_sem.at[at]).wait()

    def drain(only):
        for at, size in owed[only]:
            ref = size()
            pltpu.make_async_copy(ref, ref, send_sem.at[at]).wait()

    def src_part(d):
        return {1: 2, -1: 1, 0: slice(1, 3)}[d]

    def dst_part(d):
        return {1: 0, -1: 3, 0: slice(1, 3)}[d]

    def halo_start(field):
        out = []
        for d in DIRS:
            dx, dy = d

            def source(dx=dx, dy=dy):
                return field.at[src_part(dx), src_part(dy)]

            def target(dx=dx, dy=dy):
                return field.at[dst_part(dx), dst_part(dy)]

            at = fresh(d, source)

            @pl.when(exists[d])
            def _(d=d, source=source, target=target, at=at):
                send(source(), target(), beside[d], at)

            out.append((d, at, target))
        return out

    def halo_finish(waits):
        for (dx, dy), at, target in waits:

            @pl.when(exists[-dx, -dy])
            def _(at=at, target=target):
                arrive(target, at)

    def zero_rim(field, last):
        @pl.when(s == 0)
        def _():
            for b in range(last + 1):
                field[0, b] = jnp.zeros(field.shape[2:], field.dtype)

        @pl.when(s == n_s - 1)
        def _():
            for b in range(last + 1):
                field[last, b] = jnp.zeros(field.shape[2:], field.dtype)

        @pl.when(f == 0)
        def _():
            for a in range(last + 1):
                field[a, 0] = jnp.zeros(field.shape[2:], field.dtype)

        @pl.when(f == n_f - 1)
        def _():
            for a in range(last + 1):
                field[a, last] = jnp.zeros(field.shape[2:], field.dtype)

    vol_waits = halo_start(ext)
    zero_rim(ext, 3)
    zero_rim(extd, 3)

    loads[1].wait()
    for k in range(15):
        dz, c = k // 5, k % 5
        right = w2raw[6 * c + 3 + dz] if c < 4 else jnp.zeros((16, 64), BF16)
        w2p[k] = side_by_side(w2raw[6 * c + dz], right)
    w2p[15] = jnp.zeros((16, 128), BF16)
    half = w2p.at[pl.ds(8 * core, 8)]
    w2_flip, w2_row = fresh(None, lambda: half), fresh(None, lambda: w2g.at[core, 0 : n_x - 1])
    send(half, w2g.at[core, f], (s, flip), w2_flip)
    for to in x_ahead:
        send(half, w2g.at[core, f], (s, to), w2_row)
    w2g[core, f] = w2p[pl.ds(8 * core, 8)]

    loads[2].wait()
    crows[...] = craw[...].reshape(16 * n_f, 128).astype(F32)
    for k in range(n_f):
        cotb[k] = crows[pl.ds(k, 16, stride=n_f), :].astype(BF16)
    cot_at = fresh(None, lambda: cotb.at[0 : n_f - 1])
    for other, peer in zip(f_ahead, to_f):
        send(cotb.at[other], cotg.at[f], peer, cot_at)
    cotg[f] = cotb[f]

    loads[3].wait()
    for k in range(15):
        dz, c = k // 5, k % 5
        rows = slice(64 * dz, 64 * dz + 64)
        cols = slice(128 * c, 128 * c + 128)
        right = w1raw[6 * c + 3 + dz] if c < 4 else jnp.zeros((64, 64), BF16)
        w1f[rows, cols] = side_by_side(w1raw[6 * c + dz], right)
        back = [w1raw[3 * (8 - 2 * c) + dz]]
        back.append(w1raw[3 * (7 - 2 * c) + dz] if c < 4 else jnp.zeros((64, 64), BF16))
        w1b[rows, cols] = jnp.concatenate(back, axis=0).astype(F32).T.astype(BF16)
    ps[3, 0] = jnp.zeros((64, 128), BF16)
    pair_row = lax.broadcasted_iota(jnp.int32, (256, 128), 0)
    pair_col = lax.broadcasted_iota(jnp.int32, (256, 128), 1)
    below = pair_row - 2 * pair_col
    pairs = jnp.where((below == 0) | (below == 1), 1.0, 0.0).astype(BF16)

    def stack(field, a, b):
        planes = [field[a + i, b + j] for i in range(3) for j in range(3)]
        return jnp.concatenate(planes + [jnp.zeros((64, 256), BF16)], axis=0)

    arrive(w2g.at[core, flip], w2_flip)
    w2_pass = fresh(None, lambda: w2g.at[core, 0 : n_x - 1])
    for to in x_ahead:
        send(w2g.at[core, flip], w2g.at[core, flip], (s, to), w2_pass)
    halo_finish(vol_waits)

    wf = w1f[...]
    total = jnp.zeros((64, 128), F32)
    for a in range(2):
        for b in range(2):
            rows = jnp.dot(wf, stack(ext, a, b), preferred_element_type=F32)
            pre = shifted(rows[0:64], -1) + rows[64:128] + shifted(rows[128:192], 1)
            gate = sigmoid(pre)
            slope1[a, b] = gate * (1.0 + pre * (1.0 - gate))
            hidden = (pre * gate).astype(BF16)
            total = total + jnp.dot(hidden, pairs, preferred_element_type=F32)
    ps[1, 1] = (0.125 * total).astype(BF16)

    pool_at = fresh(None, lambda: ps.at[0:4, 0:2])
    for d in DIRS:
        send(ps.at[1, 1], ps.at[1 - d[0], 1 - d[1]], beside[d], pool_at)

    arrive(lambda: w2g.at[core, 0 : n_x - 1], w2_row)
    arrive(lambda: w2g.at[core, 0 : n_x - 1], w2_pass)
    w2_twin = fresh(None, lambda: w2g.at[core])
    send(w2g.at[core], w2g.at[core], twin, w2_twin)
    arrive(lambda: cotg.at[0 : n_f - 1], cot_at)
    arrive(lambda: w2g.at[1 - core], w2_twin)
    w2 = []
    for dz in range(3):
        tiles = [
            w2g[k // 8, :, k % 8].reshape(16 * n_f, 128) for k in range(5 * dz, 5 * dz + 5)
        ]
        w2.append(jnp.concatenate(tiles, axis=1))
        for c in range(5):
            w2t[dz, 128 * c : 128 * c + 128] = tiles[c].astype(F32).T.astype(BF16)

    arrive(lambda: ps.at[0:4, 0:2], pool_at)
    zero_rim(ps, 2)

    around = jnp.concatenate(
        [ps[i, j] for i in range(3) for j in range(3)] + [ps[3, 0]], axis=0
    )
    rows = [jnp.dot(w, around, preferred_element_type=F32) for w in w2]
    pre = shifted(rows[0], -1) + rows[1] + shifted(rows[2], 1)
    gate = sigmoid(pre)
    down = cotg[...].reshape(128, 128).astype(F32) * (gate * (1.0 + pre * (1.0 - gate)))
    down_own = down.astype(BF16)

    rows = [jnp.dot(w2t[dz], down_own, preferred_element_type=F32) for dz in range(3)]
    share = shifted(rows[0], 1) + rows[1] + shifted(rows[2], -1)
    down_at = fresh(None, lambda: give.at[0:8])
    for dx, dy in DIRS:
        slot = 3 * (dx + 1) + dy + 1
        give[slot] = share[64 * slot : 64 * slot + 64].astype(BF16)
        send(give.at[slot], take.at[1 - dx, 1 - dy], beside[dx, dy], down_at)
    own_share = share[256:320]
    featb[0] = (pre * gate).astype(BF16).reshape(n_f, 16, 128)

    feat_at = fresh(None, lambda: featb.at[0, 0 : n_f - 1])
    for other, peer in zip(f_ahead, to_f):
        send(featb.at[0, other], featb.at[1, f], peer, feat_at)
    featb[1, f] = featb[0, f]

    lhs = jnp.concatenate(
        [shifted(down, 1).astype(BF16), down_own, shifted(down, -1).astype(BF16)], axis=0
    )
    terms = nt_dot(lhs, around)

    def deal(values, height, per, step, put):
        for g in range(n_f):
            tiles = [
                values[per * g + step * r : per * g + step * r + height, 128 * c : 128 * c + 128]
                for r in range(3)
                for c in range(5)
            ]
            tiles.append(jnp.zeros((height, 128), F32))
            put(g, jnp.concatenate(tiles, axis=0).astype(BF16))

    def put_bottom(g, piece):
        s_gb[g] = piece

    deal(terms, 16, 16, 128, put_bottom)

    def exchange(ref, mine, peers, only):
        at = fresh(only, lambda: ref.at[0 : len(peers)])
        for peer in peers:
            send(ref.at[mine], ref.at[mine], peer, at)
        return at, lambda: ref.at[0 : len(peers)]

    def scatter(out, into, mine, peers, theirs, only):
        at = fresh(only, lambda: out.at[0 : len(peers)])
        for peer, other in zip(peers, theirs):
            send(out.at[other], into.at[mine], peer, at)
        return at, lambda: into.at[0 : len(peers)]

    def finish(waits):
        for at, ref in waits:
            arrive(ref, at)

    def summed(ref, count):
        value = ref[0].astype(F32)
        for k in range(1, count):
            value = value + ref[k].astype(F32)
        return value.astype(BF16)

    s_waits = []
    s_twin = fresh(1, lambda: s_gb)

    @pl.when(second)
    def _():
        send(s_gb, s_cb, twin, s_twin)

    @pl.when(first)
    def _():
        arrive(s_cb, s_twin)
        s_pb[...] = (s_gb[...].astype(F32) + s_cb[...].astype(F32)).astype(BF16)
        s_fb[f] = s_pb[f]
        s_waits.append(scatter(s_pb, s_fb, f, to_f, f_ahead, 0))

    arrive(lambda: give.at[0:8], down_at)
    zero_rim(take, 2)
    pool_grad = own_share
    for dx, dy in DIRS:
        pool_grad = pool_grad + take[1 - dx, 1 - dy].astype(F32)
    pool_grad = 0.125 * pool_grad
    high = pool_grad.astype(BF16)
    low = (pool_grad - high.astype(F32)).astype(BF16)
    spread = nt_dot(jnp.concatenate([high, low], axis=0), pairs)
    spread = spread[0:64] + spread[64:128]
    for a in range(2):
        for b in range(2):
            extd[a + 1, b + 1] = (spread * slope1[a, b]).astype(BF16)

    fd_waits = halo_start(extd)

    terms = jnp.zeros((192, 640), F32)
    for a in range(2):
        for b in range(2):
            own = extd[a + 1, b + 1]
            wide = own.astype(F32)
            lhs = jnp.concatenate(
                [shifted(wide, 1).astype(BF16), own, shifted(wide, -1).astype(BF16)], axis=0
            )
            terms = terms + nt_dot(lhs, stack(ext, a, b))

    per_peer = 16 // n_xy

    def put_fine(g, piece):
        for h in range(2):
            at = 2 * g + h
            row = 64 * (at % per_peer)
            f_gb[at // per_peer, row : row + 64] = piece[64 * h : 64 * h + 64]

        def part(buffer):
            if per_peer == 1:
                return buffer.at[2 * g : 2 * g + 2]
            return buffer.at[2 * g // per_peer, pl.ds(64 * (2 * g % per_peer), 128)]

        @pl.when(first)
        def _():
            send(part(f_gb), part(f_cb), twin, f_twin)

    f_twin = fresh(0, lambda: f_gb)
    deal(terms, 8, 24, 8, put_fine)
    plane_waits, z_waits = [], []

    @pl.when(second)
    def _():
        arrive(f_cb, f_twin)
        f_pb[...] = (f_gb[...].astype(F32) + f_cb[...].astype(F32)).astype(BF16)
        f_xr[at_xy] = f_pb[at_xy]
        plane_waits.append(scatter(f_pb, f_xr, at_xy, to_plane, plane_ahead, 1))

    @pl.when(first)
    def _():
        finish(s_waits)
        s_zr[zh] = summed(s_fb, n_f)
        z_waits.append(exchange(s_zr, zh, to_z, 0))

    depth_waits, y_waits = [], []

    @pl.when(second)
    def _():
        finish(plane_waits)
        f_zr[at_z] = summed(f_xr, n_xy)
        depth_waits.append(exchange(f_zr, at_z, to_depth, 1))

    @pl.when(first)
    def _():
        finish(z_waits)
        s_yr[y] = summed(s_zr, n_z)
        y_waits.append(exchange(s_yr, y, to_y, 0))

    halo_finish(fd_waits)
    wb = w1b[...]
    for a in range(2):
        for b in range(2):
            rows = jnp.dot(wb, stack(extd, a, b), preferred_element_type=F32)
            plane = shifted(rows[0:64], 1) + rows[64:128] + shifted(rows[128:192], -1)
            for h in range(2):
                vrows[h, pl.ds(2 * a + b, 64, stride=4), :] = plane[:, 128 * h : 128 * h + 128]

    for c in range(64):
        for a in range(2):
            for h in range(2):
                vgrad_out[c, a, :, 128 * h : 128 * h + 128] = vrows[
                    h, 4 * c + 2 * a : 4 * c + 2 * a + 2
                ].astype(BF16)

    arrive(lambda: featb.at[1, 0 : n_f - 1], feat_at)
    for k in range(n_f):
        crows[pl.ds(k, 16, stride=n_f), :] = featb[1, k].astype(F32)
    feat_out[...] = crows[...].reshape(16, 1, n_f, 128).astype(BF16)

    s_last, f_last = fresh(0, lambda: s_os), fresh(1, lambda: f_ag)

    @pl.when(first)
    def _():
        finish(y_waits)
        s_os[...] = summed(s_yr, n_y)
        send(s_os, s_os, twin, s_last)

    @pl.when(second)
    def _():
        finish(depth_waits)
        f_ag[at_xy] = summed(f_zr, 2 * n_z)
        finish([exchange(f_ag, at_xy, to_plane, 1)])
        send(f_ag, f_ag, twin, f_last)
        arrive(s_os, s_last)

    @pl.when(first)
    def _():
        arrive(f_ag, f_last)

    os_out[...] = s_os[...]
    ag_out[...] = f_ag[...]

    assert len(used) <= N_SEMS
    drain(None)
    for d in DIRS:

        @pl.when(exists[d])
        def _(d=d):
            drain(d)

    @pl.when(first)
    def _():
        drain(0)

    @pl.when(second)
    def _():
        drain(1)


def unpack(n_f, scales, feat_in, vgrad_in, ag_in, os_in, feat_out, vgrad_out, g1_out, g2_out):
    fine_scale, bottom_scale = scales
    feat_out[...] = feat_in[...]
    vgrad_out[...] = vgrad_in[...]
    for k in range(15):
        dz, c = k // 5, k % 5
        tile = os_in[16 * k : 16 * k + 16].astype(F32) * bottom_scale
        g2_out[6 * c + dz] = tile[:, 0:64]
        if c < 4:
            g2_out[6 * c + 3 + dz] = pltpu.roll(tile, 64, 1)[:, 0:64]
    for g in range(n_f):
        per_peer = 16 // ag_in.shape[0]
        both = []
        for at in (2 * g, 2 * g + 1):
            start = 64 * (at % per_peer)
            both.append(ag_in[at // per_peer, start : start + 64].astype(F32) * fine_scale)
        for k in range(15):
            row = 24 * g + 8 * (k // 5)
            dz, o = row // 64, row % 64
            c = k % 5
            tile = both[k // 8][8 * (k % 8) : 8 * (k % 8) + 8]
            g1_out[6 * c + dz, o : o + 8] = tile[:, 0:64]
            if c < 4:
                g1_out[6 * c + 3 + dz, o : o + 8] = pltpu.roll(tile, 64, 1)[:, 0:64]


def local(sizes, volume, first_weight, second_weight, cotangent):
    n_s, n_f, n_y, n_z = sizes
    n_xy = n_f // 2 * n_y
    scales = (
        1.0 / float(n_s * 2 * n_f * 2 * 256) ** 0.5,
        1.0 / float(n_s * n_f * 128) ** 0.5,
    )
    vmem = pl.BlockSpec(memory_space=pltpu.VMEM)
    whole = pl.BlockSpec(memory_space=pltpu.HBM)
    operands = (volume, cotangent, first_weight, second_weight)
    shape = jax.ShapeDtypeStruct
    features, volume_grad, fine, bottom = pl.pallas_call(
        functools.partial(kernel, sizes),
        out_shape=(
            shape((16, 1, n_f, 128), BF16),
            shape((64, 2, 2, 256), BF16),
            shape((n_xy, 1024 // n_xy, 128), BF16),
            shape((256, 128), BF16),
        ),
        in_specs=[whole] * 4,
        out_specs=(vmem,) * 4,
        scratch_shapes=[
            pltpu.VMEM((64, 2, 2, 256), BF16),
            pltpu.VMEM((16, 1, n_f, 128), BF16),
            pltpu.VMEM((27, 64, 64), BF16),
            pltpu.VMEM((27, 16, 64), BF16),
            pltpu.VMEM((2, 256, 128), F32),
            pltpu.VMEM((16 * n_f, 128), F32),
            pltpu.VMEM((n_f, 16, 128), BF16),
            pltpu.VMEM((192, 640), BF16),
            pltpu.VMEM((192, 640), BF16),
            pltpu.VMEM((16, 16, 128), BF16),
            pltpu.VMEM((4, 4, 64, 256), BF16),
            pltpu.VMEM((4, 4, 64, 256), BF16),
            pltpu.VMEM((2, 2, 64, 256), F32),
            pltpu.VMEM((n_f, 16, 128), BF16),
            pltpu.VMEM((2, n_f, 8, 16, 128), BF16),
            pltpu.VMEM((3, 640, 128), BF16),
            pltpu.VMEM((4, 3, 64, 128), BF16),
            pltpu.VMEM((9, 64, 128), BF16),
            pltpu.VMEM((3, 3, 64, 128), BF16),
            pltpu.VMEM((2, n_f, 16, 128), BF16),
            pltpu.VMEM((n_f, 256, 128), BF16),
            pltpu.VMEM((n_f, 256, 128), BF16),
            pltpu.VMEM((n_f, 256, 128), BF16),
            pltpu.VMEM((n_f, 256, 128), BF16),
            pltpu.VMEM((n_y, 256, 128), BF16),
            pltpu.VMEM((n_z, 256, 128), BF16),
            pltpu.VMEM((256, 128), BF16),
            pltpu.VMEM((n_xy, 1024 // n_xy, 128), BF16),
            pltpu.VMEM((n_xy, 1024 // n_xy, 128), BF16),
            pltpu.VMEM((n_xy, 1024 // n_xy, 128), BF16),
            pltpu.VMEM((n_xy, 1024 // n_xy, 128), BF16),
            pltpu.VMEM((2 * n_z, 1024 // n_xy, 128), BF16),
            pltpu.VMEM((n_xy, 1024 // n_xy, 128), BF16),
            pltpu.SemaphoreType.DMA((4,)),
            pltpu.SemaphoreType.DMA((N_SEMS,)),
            pltpu.SemaphoreType.DMA((N_SEMS,)),
        ],
        compiler_params=pltpu.CompilerParams(
            collective_id=0, has_side_effects=True, vmem_limit_bytes=24 * 1024 * 1024
        ),
        name="block",
    )(*(pltpu.with_memory_space_constraint(v, pltpu.HBM) for v in operands))
    return pl.pallas_call(
        functools.partial(unpack, n_f, scales),
        out_shape=(
            shape((16, 1, n_f, 128), BF16),
            shape((64, 2, 2, 256), BF16),
            shape((27, 64, 64), F32),
            shape((27, 16, 64), F32),
        ),
        in_specs=[vmem] * 4,
        out_specs=(vmem,) * 4,
        compiler_params=pltpu.CompilerParams(vmem_limit_bytes=24 * 1024 * 1024),
        name="unpack",
    )(features, volume_grad, fine, bottom)


def solution(mesh):
    n_s, n_f = mesh.shape["space"], mesh.shape["filt"]
    n_z = 4 if n_s % 8 == 0 else 1
    sizes = (n_s, n_f, n_s // (2 * n_z), n_z)
    placed = (
        P(None, "space", "filt", None),
        P(),
        P(None, "filt", None),
        P("filt", "space", None, None),
    )
    return jax.shard_map(
        functools.partial(local, sizes),
        mesh=mesh,
        in_specs=placed,
        out_specs=(
            P("filt", "space", None, None),
            P(None, "space", "filt", None),
            P(),
            P(None, "filt", None),
        ),
        check_vma=False,
    )
```

```python
import functools

import jax
import jax.numpy as jnp
from jax import lax
from jax.experimental import pallas as pl
from jax.experimental.pallas import tpu as pltpu
from jax.sharding import PartitionSpec as P

MESH = pl.DeviceIdType.MESH
F32 = jnp.float32
BF16 = jnp.bfloat16
DIRS = [(-1, -1), (-1, 1), (1, -1), (1, 1), (-1, 0), (1, 0), (0, -1), (0, 1)]
N_SEMS = 34


def far_first(*rings):
    offsets = [()]
    for length in rings:
        offsets = [o + (k,) for o in offsets for k in range(length)]
    hops = [sum(min(k, n - k) for k, n in zip(o, rings)) for o in offsets]
    order = sorted(range(1, len(offsets)), key=lambda i: -hops[i])
    return [offsets[i] for i in order]


def sigmoid(v):
    return 1.0 / (1.0 + jnp.exp(-v))


def shifted(values, by):
    if by == 0:
        return values
    length = values.shape[1]
    lane = lax.broadcasted_iota(jnp.int32, values.shape, 1)
    if by == 1:
        return jnp.where(lane == length - 1, 0.0, pltpu.roll(values, length - 1, 1))
    return jnp.where(lane == 0, 0.0, pltpu.roll(values, 1, 1))


def nt_dot(a, b):
    return lax.dot_general(a, b, (((1,), (1,)), ((), ())), preferred_element_type=F32)


def side_by_side(left, right):
    return jnp.concatenate([left, right], axis=1)


def kernel(
    sizes,
    vol_hbm,
    cot_hbm,
    w1_hbm,
    w2_hbm,
    feat_out,
    vgrad_out,
    ag_out,
    os_out,
    vraw,
    craw,
    w1raw,
    w2raw,
    vrows,
    crows,
    cotb,
    w1f,
    w1b,
    w2p,
    ext,
    extd,
    slope1,
    cotg,
    w2g,
    w2t,
    ps,
    give,
    take,
    featb,
    s_gb,
    s_cb,
    s_pb,
    s_fb,
    s_yr,
    s_zr,
    s_os,
    f_gb,
    f_cb,
    f_pb,
    f_xr,
    f_zr,
    f_ag,
    load_sem,
    send_sem,
    recv_sem,
):
    n_s, n_f, n_y, n_z = sizes
    s = lax.axis_index("space")
    f = lax.axis_index("filt")
    core = lax.rem(s, 2)
    zh = lax.rem(s // 2, n_z)
    y = s // (2 * n_z)

    loads = []
    for at, (whole, raw) in enumerate(
        ((vol_hbm, vraw), (w2_hbm, w2raw), (cot_hbm, craw), (w1_hbm, w1raw))
    ):
        load = pltpu.make_async_copy(whole, raw, load_sem.at[at])
        load.start()
        loads.append(load)

    def near(dx, dy):
        return (lax.rem(s + dx + n_s, n_s), lax.rem(f + dy + n_f, n_f))

    twin = (s + 1 - 2 * core, f)
    n_x = n_f // 2
    n_xy = n_x * n_y
    x, zl = lax.rem(f, n_x), f // n_x
    at_xy = y * n_x + x
    at_z = 2 * zh + zl

    def device(y_to, zh_to, zl_to, x_to):
        return ((y_to * n_z + zh_to) * 2 + core, zl_to * n_x + x_to)

    def turned_by(position, by, length):
        return position if by == 0 else lax.rem(position + by, length)

    to_f, f_ahead = [], []
    for p, q in far_first(2, n_x):
        to_f.append(device(y, zh, turned_by(zl, p, 2), turned_by(x, q, n_x)))
        f_ahead.append(to_f[-1][1])
    to_y = [device(turned_by(y, p, n_y), zh, zl, x) for (p,) in far_first(n_y)]
    to_z = [device(y, turned_by(zh, p, n_z), zl, x) for (p,) in far_first(n_z)]
    to_plane, plane_ahead = [], []
    for p, q in far_first(n_y, n_x):
        y_to, x_to = turned_by(y, p, n_y), turned_by(x, q, n_x)
        to_plane.append(device(y_to, zh, zl, x_to))
        plane_ahead.append(y_to * n_x + x_to)
    to_depth = []
    for (p,) in far_first(2 * n_z):
        to = turned_by(at_z, p, 2 * n_z)
        to_depth.append(device(y, to // 2, lax.rem(to, 2), x))
    first, second = core == 0, core == 1
    in_s = {-1: s > 0, 0: s >= 0, 1: s < n_s - 1}
    in_f = {-1: f > 0, 0: f >= 0, 1: f < n_f - 1}
    exists = {(dx, dy): in_s[dx] & in_f[dy] for dx, dy in DIRS}
    beside = {d: near(*d) for d in DIRS}
    flip = (1 - zl) * n_x + x
    x_ahead = [zl * n_x + lax.rem(x + j, n_x) for j in range(1, n_x)]

    peers = [beside[d] for d in DIRS] + to_f + to_plane + to_depth
    barrier = pltpu.get_barrier_semaphore()
    for peer in peers:
        pl.semaphore_signal(barrier, inc=1, device_id=peer, device_id_type=MESH)

    loads[0].wait()
    for c in range(64):
        for a in range(2):
            for h in range(2):
                vrows[h, 4 * c + 2 * a : 4 * c + 2 * a + 2] = vraw[
                    c, a, :, 128 * h : 128 * h + 128
                ].astype(F32)
    for a in range(2):
        for b in range(2):
            for h in range(2):
                ext[a + 1, b + 1, :, 128 * h : 128 * h + 128] = vrows[
                    h, pl.ds(2 * a + b, 64, stride=4), :
                ].astype(BF16)
    pl.semaphore_wait(barrier, len(peers))

    used = []
    owed = {}

    def fresh(only, size):
        at = len(used)
        used.append(at)
        owed.setdefault(only, []).append((at, size))
        return at

    def send(src, dst, device, at):
        pltpu.make_async_remote_copy(
            src_ref=src,
            dst_ref=dst,
            send_sem=send_sem.at[at],
            recv_sem=recv_sem.at[at],
            device_id=device,
            device_id_type=MESH,
        ).start()

    def arrive(ref, at):
        ref = ref() if callable(ref) else ref
        pltpu.make_async_copy(ref, ref, recv_sem.at[at]).wait()

    def drain(only):
        for at, size in owed[only]:
            ref = size()
            pltpu.make_async_copy(ref, ref, send_sem.at[at]).wait()

    def src_part(d):
        return {1: 2, -1: 1, 0: slice(1, 3)}[d]

    def dst_part(d):
        return {1: 0, -1: 3, 0: slice(1, 3)}[d]

    def halo_start(field):
        out = []
        for d in DIRS:
            dx, dy = d

            def source(dx=dx, dy=dy):
                return field.at[src_part(dx), src_part(dy)]

            def target(dx=dx, dy=dy):
                return field.at[dst_part(dx), dst_part(dy)]

            at = fresh(d, source)

            @pl.when(exists[d])
            def _(d=d, source=source, target=target, at=at):
                send(source(), target(), beside[d], at)

            out.append((d, at, target))
        return out

    def halo_finish(waits):
        for (dx, dy), at, target in waits:

            @pl.when(exists[-dx, -dy])
            def _(at=at, target=target):
                arrive(target, at)

    def zero_rim(field, last):
        @pl.when(s == 0)
        def _():
            for b in range(last + 1):
                field[0, b] = jnp.zeros(field.shape[2:], field.dtype)

        @pl.when(s == n_s - 1)
        def _():
            for b in range(last + 1):
                field[last, b] = jnp.zeros(field.shape[2:], field.dtype)

        @pl.when(f == 0)
        def _():
            for a in range(last + 1):
                field[a, 0] = jnp.zeros(field.shape[2:], field.dtype)

        @pl.when(f == n_f - 1)
        def _():
            for a in range(last + 1):
                field[a, last] = jnp.zeros(field.shape[2:], field.dtype)

    vol_waits = halo_start(ext)
    zero_rim(ext, 3)
    zero_rim(extd, 3)

    loads[1].wait()
    for k in range(15):
        dz, c = k // 5, k % 5
        right = w2raw[6 * c + 3 + dz] if c < 4 else jnp.zeros((16, 64), BF16)
        w2p[k] = side_by_side(w2raw[6 * c + dz], right)
    w2p[15] = jnp.zeros((16, 128), BF16)
    half = w2p.at[pl.ds(8 * core, 8)]
    w2_flip, w2_row = fresh(None, lambda: half), fresh(None, lambda: w2g.at[core, 0 : n_x - 1])
    send(half, w2g.at[core, f], (s, flip), w2_flip)
    for to in x_ahead:
        send(half, w2g.at[core, f], (s, to), w2_row)
    w2g[core, f] = w2p[pl.ds(8 * core, 8)]

    loads[2].wait()
    crows[...] = craw[...].reshape(16 * n_f, 128).astype(F32)
    for k in range(n_f):
        cotb[k] = crows[pl.ds(k, 16, stride=n_f), :].astype(BF16)
    cot_at = fresh(None, lambda: cotb.at[0 : n_f - 1])
    for other, peer in zip(f_ahead, to_f):
        send(cotb.at[other], cotg.at[f], peer, cot_at)
    cotg[f] = cotb[f]

    loads[3].wait()
    for k in range(15):
        dz, c = k // 5, k % 5
        rows = slice(64 * dz, 64 * dz + 64)
        cols = slice(128 * c, 128 * c + 128)
        right = w1raw[6 * c + 3 + dz] if c < 4 else jnp.zeros((64, 64), BF16)
        w1f[rows, cols] = side_by_side(w1raw[6 * c + dz], right)
        back = [w1raw[3 * (8 - 2 * c) + dz]]
        back.append(w1raw[3 * (7 - 2 * c) + dz] if c < 4 else jnp.zeros((64, 64), BF16))
        w1b[rows, cols] = jnp.concatenate(back, axis=0).astype(F32).T.astype(BF16)
    ps[3, 0] = jnp.zeros((64, 128), BF16)
    pair_row = lax.broadcasted_iota(jnp.int32, (256, 128), 0)
    pair_col = lax.broadcasted_iota(jnp.int32, (256, 128), 1)
    below = pair_row - 2 * pair_col
    pairs = jnp.where((below == 0) | (below == 1), 1.0, 0.0).astype(BF16)

    def stack(field, a, b):
        planes = [field[a + i, b + j] for i in range(3) for j in range(3)]
        return jnp.concatenate(planes + [jnp.zeros((64, 256), BF16)], axis=0)

    arrive(w2g.at[core, flip], w2_flip)
    w2_pass = fresh(None, lambda: w2g.at[core, 0 : n_x - 1])
    for to in x_ahead:
        send(w2g.at[core, flip], w2g.at[core, flip], (s, to), w2_pass)
    halo_finish(vol_waits)

    wf = w1f[...]
    total = jnp.zeros((64, 128), F32)
    for a in range(2):
        for b in range(2):
            rows = jnp.dot(wf, stack(ext, a, b), preferred_element_type=F32)
            pre = shifted(rows[0:64], -1) + rows[64:128] + shifted(rows[128:192], 1)
            gate = sigmoid(pre)
            slope1[a, b] = pre
            hidden = (pre * gate).astype(BF16)
            total = total + jnp.dot(hidden, pairs, preferred_element_type=F32)
    ps[1, 1] = (0.125 * total).astype(BF16)

    pool_at = fresh(None, lambda: ps.at[0:4, 0:2])
    for d in DIRS:
        send(ps.at[1, 1], ps.at[1 - d[0], 1 - d[1]], beside[d], pool_at)

    for a in range(2):
        for b in range(2):
            pre = slope1[a, b]
            gate = sigmoid(pre)
            slope1[a, b] = gate * (1.0 + pre * (1.0 - gate))

    arrive(lambda: w2g.at[core, 0 : n_x - 1], w2_row)
    arrive(lambda: w2g.at[core, 0 : n_x - 1], w2_pass)
    w2_twin = fresh(None, lambda: w2g.at[core])
    send(w2g.at[core], w2g.at[core], twin, w2_twin)
    arrive(lambda: cotg.at[0 : n_f - 1], cot_at)
    arrive(lambda: w2g.at[1 - core], w2_twin)
    w2 = []
    for dz in range(3):
        tiles = [
            w2g[k // 8, :, k % 8].reshape(16 * n_f, 128) for k in range(5 * dz, 5 * dz + 5)
        ]
        w2.append(jnp.concatenate(tiles, axis=1))
        for c in range(5):
            w2t[dz, 128 * c : 128 * c + 128] = tiles[c].astype(F32).T.astype(BF16)

    arrive(lambda: ps.at[0:4, 0:2], pool_at)
    zero_rim(ps, 2)

    around = jnp.concatenate(
        [ps[i, j] for i in range(3) for j in range(3)] + [ps[3, 0]], axis=0
    )
    rows = [jnp.dot(w, around, preferred_element_type=F32) for w in w2]
    pre = shifted(rows[0], -1) + rows[1] + shifted(rows[2], 1)
    gate = sigmoid(pre)
    down = cotg[...].reshape(128, 128).astype(F32) * (gate * (1.0 + pre * (1.0 - gate)))
    down_own = down.astype(BF16)

    rows = [jnp.dot(w2t[dz], down_own, preferred_element_type=F32) for dz in range(3)]
    share = shifted(rows[0], 1) + rows[1] + shifted(rows[2], -1)
    down_at = fresh(None, lambda: give.at[0:8])
    for dx, dy in DIRS:
        slot = 3 * (dx + 1) + dy + 1
        give[slot] = share[64 * slot : 64 * slot + 64].astype(BF16)
        send(give.at[slot], take.at[1 - dx, 1 - dy], beside[dx, dy], down_at)
    own_share = share[256:320]
    featb[0] = (pre * gate).astype(BF16).reshape(n_f, 16, 128)

    feat_at = fresh(None, lambda: featb.at[0, 0 : n_f - 1])
    for other, peer in zip(f_ahead, to_f):
        send(featb.at[0, other], featb.at[1, f], peer, feat_at)
    featb[1, f] = featb[0, f]

    lhs = jnp.concatenate(
        [shifted(down, 1).astype(BF16), down_own, shifted(down, -1).astype(BF16)], axis=0
    )
    terms = nt_dot(lhs, around)

    def deal(values, height, per, step, put):
        for g in range(n_f):
            tiles = [
                values[per * g + step * r : per * g + step * r + height, 128 * c : 128 * c + 128]
                for r in range(3)
                for c in range(5)
            ]
            tiles.append(jnp.zeros((height, 128), F32))
            put(g, jnp.concatenate(tiles, axis=0).astype(BF16))

    s_twin = fresh(1, lambda: s_gb)

    def put_bottom(g, piece):
        s_gb[g] = piece

        @pl.when(second)
        def _():
            send(s_gb.at[g], s_cb.at[g], twin, s_twin)

    deal(terms, 16, 16, 128, put_bottom)

    def exchange(ref, mine, peers, only):
        at = fresh(only, lambda: ref.at[0 : len(peers)])
        for peer in peers:
            send(ref.at[mine], ref.at[mine], peer, at)
        return at, lambda: ref.at[0 : len(peers)]

    def scatter(out, into, mine, peers, theirs, only):
        at = fresh(only, lambda: out.at[0 : len(peers)])
        for peer, other in zip(peers, theirs):
            send(out.at[other], into.at[mine], peer, at)
        return at, lambda: into.at[0 : len(peers)]

    def finish(waits):
        for at, ref in waits:
            arrive(ref, at)

    def summed(ref, count):
        value = ref[0].astype(F32)
        for k in range(1, count):
            value = value + ref[k].astype(F32)
        return value.astype(BF16)

    s_waits = []
    @pl.when(first)
    def _():
        arrive(s_cb, s_twin)
        s_pb[...] = (s_gb[...].astype(F32) + s_cb[...].astype(F32)).astype(BF16)
        s_fb[f] = s_pb[f]
        s_waits.append(scatter(s_pb, s_fb, f, to_f, f_ahead, 0))

    arrive(lambda: give.at[0:8], down_at)
    zero_rim(take, 2)
    pool_grad = own_share
    for dx, dy in DIRS:
        pool_grad = pool_grad + take[1 - dx, 1 - dy].astype(F32)
    pool_grad = 0.125 * pool_grad
    high = pool_grad.astype(BF16)
    low = (pool_grad - high.astype(F32)).astype(BF16)
    spread = nt_dot(jnp.concatenate([high, low], axis=0), pairs)
    spread = spread[0:64] + spread[64:128]
    for a in range(2):
        for b in range(2):
            extd[a + 1, b + 1] = (spread * slope1[a, b]).astype(BF16)

    fd_waits = halo_start(extd)

    terms = jnp.zeros((192, 640), F32)
    for a in range(2):
        for b in range(2):
            own = extd[a + 1, b + 1]
            wide = own.astype(F32)
            lhs = jnp.concatenate(
                [shifted(wide, 1).astype(BF16), own, shifted(wide, -1).astype(BF16)], axis=0
            )
            terms = terms + nt_dot(lhs, stack(ext, a, b))

    per_peer = 16 // n_xy

    def put_fine(g, piece):
        for h in range(2):
            at = 2 * g + h
            row = 64 * (at % per_peer)
            f_gb[at // per_peer, row : row + 64] = piece[64 * h : 64 * h + 64]

        def part(buffer):
            if per_peer == 1:
                return buffer.at[2 * g : 2 * g + 2]
            return buffer.at[2 * g // per_peer, pl.ds(64 * (2 * g % per_peer), 128)]

        @pl.when(first)
        def _():
            send(part(f_gb), part(f_cb), twin, f_twin)

    f_twin = fresh(0, lambda: f_gb)
    deal(terms, 8, 24, 8, put_fine)
    plane_waits, z_waits = [], []

    @pl.when(second)
    def _():
        arrive(f_cb, f_twin)
        f_pb[...] = (f_gb[...].astype(F32) + f_cb[...].astype(F32)).astype(BF16)
        f_xr[at_xy] = f_pb[at_xy]
        plane_waits.append(scatter(f_pb, f_xr, at_xy, to_plane, plane_ahead, 1))

    @pl.when(first)
    def _():
        finish(s_waits)
        s_zr[zh] = summed(s_fb, n_f)
        z_waits.append(exchange(s_zr, zh, to_z, 0))

    depth_waits, y_waits = [], []

    @pl.when(second)
    def _():
        finish(plane_waits)
        f_zr[at_z] = summed(f_xr, n_xy)
        depth_waits.append(exchange(f_zr, at_z, to_depth, 1))

    @pl.when(first)
    def _():
        finish(z_waits)
        s_yr[y] = summed(s_zr, n_z)
        y_waits.append(exchange(s_yr, y, to_y, 0))

    halo_finish(fd_waits)
    wb = w1b[...]
    for a in range(2):
        for b in range(2):
            rows = jnp.dot(wb, stack(extd, a, b), preferred_element_type=F32)
            plane = shifted(rows[0:64], 1) + rows[64:128] + shifted(rows[128:192], -1)
            for h in range(2):
                vrows[h, pl.ds(2 * a + b, 64, stride=4), :] = plane[:, 128 * h : 128 * h + 128]

    for c in range(64):
        for a in range(2):
            for h in range(2):
                vgrad_out[c, a, :, 128 * h : 128 * h + 128] = vrows[
                    h, 4 * c + 2 * a : 4 * c + 2 * a + 2
                ].astype(BF16)

    arrive(lambda: featb.at[1, 0 : n_f - 1], feat_at)
    for k in range(n_f):
        crows[pl.ds(k, 16, stride=n_f), :] = featb[1, k].astype(F32)
    feat_out[...] = crows[...].reshape(16, 1, n_f, 128).astype(BF16)

    s_last, f_last = fresh(0, lambda: s_os), fresh(1, lambda: f_ag)

    @pl.when(first)
    def _():
        finish(y_waits)
        s_os[...] = summed(s_yr, n_y)
        send(s_os, s_os, twin, s_last)

    @pl.when(second)
    def _():
        finish(depth_waits)
        f_ag[at_xy] = summed(f_zr, 2 * n_z)
        finish([exchange(f_ag, at_xy, to_plane, 1)])
        send(f_ag, f_ag, twin, f_last)
        arrive(s_os, s_last)

    @pl.when(first)
    def _():
        arrive(f_ag, f_last)

    os_out[...] = s_os[...]
    ag_out[...] = f_ag[...]

    assert len(used) <= N_SEMS
    drain(None)
    for d in DIRS:

        @pl.when(exists[d])
        def _(d=d):
            drain(d)

    @pl.when(first)
    def _():
        drain(0)

    @pl.when(second)
    def _():
        drain(1)


def unpack(n_f, scales, feat_in, vgrad_in, ag_in, os_in, feat_out, vgrad_out, g1_out, g2_out):
    fine_scale, bottom_scale = scales
    feat_out[...] = feat_in[...]
    vgrad_out[...] = vgrad_in[...]
    for k in range(15):
        dz, c = k // 5, k % 5
        tile = os_in[16 * k : 16 * k + 16].astype(F32) * bottom_scale
        g2_out[6 * c + dz] = tile[:, 0:64]
        if c < 4:
            g2_out[6 * c + 3 + dz] = pltpu.roll(tile, 64, 1)[:, 0:64]
    for g in range(n_f):
        per_peer = 16 // ag_in.shape[0]
        both = []
        for at in (2 * g, 2 * g + 1):
            start = 64 * (at % per_peer)
            both.append(ag_in[at // per_peer, start : start + 64].astype(F32) * fine_scale)
        for k in range(15):
            row = 24 * g + 8 * (k // 5)
            dz, o = row // 64, row % 64
            c = k % 5
            tile = both[k // 8][8 * (k % 8) : 8 * (k % 8) + 8]
            g1_out[6 * c + dz, o : o + 8] = tile[:, 0:64]
            if c < 4:
                g1_out[6 * c + 3 + dz, o : o + 8] = pltpu.roll(tile, 64, 1)[:, 0:64]


def local(sizes, volume, first_weight, second_weight, cotangent):
    n_s, n_f, n_y, n_z = sizes
    n_xy = n_f // 2 * n_y
    scales = (
        1.0 / float(n_s * 2 * n_f * 2 * 256) ** 0.5,
        1.0 / float(n_s * n_f * 128) ** 0.5,
    )
    vmem = pl.BlockSpec(memory_space=pltpu.VMEM)
    whole = pl.BlockSpec(memory_space=pltpu.HBM)
    operands = (volume, cotangent, first_weight, second_weight)
    shape = jax.ShapeDtypeStruct
    features, volume_grad, fine, bottom = pl.pallas_call(
        functools.partial(kernel, sizes),
        out_shape=(
            shape((16, 1, n_f, 128), BF16),
            shape((64, 2, 2, 256), BF16),
            shape((n_xy, 1024 // n_xy, 128), BF16),
            shape((256, 128), BF16),
        ),
        in_specs=[whole] * 4,
        out_specs=(vmem,) * 4,
        scratch_shapes=[
            pltpu.VMEM((64, 2, 2, 256), BF16),
            pltpu.VMEM((16, 1, n_f, 128), BF16),
            pltpu.VMEM((27, 64, 64), BF16),
            pltpu.VMEM((27, 16, 64), BF16),
            pltpu.VMEM((2, 256, 128), F32),
            pltpu.VMEM((16 * n_f, 128), F32),
            pltpu.VMEM((n_f, 16, 128), BF16),
            pltpu.VMEM((192, 640), BF16),
            pltpu.VMEM((192, 640), BF16),
            pltpu.VMEM((16, 16, 128), BF16),
            pltpu.VMEM((4, 4, 64, 256), BF16),
            pltpu.VMEM((4, 4, 64, 256), BF16),
            pltpu.VMEM((2, 2, 64, 256), F32),
            pltpu.VMEM((n_f, 16, 128), BF16),
            pltpu.VMEM((2, n_f, 8, 16, 128), BF16),
            pltpu.VMEM((3, 640, 128), BF16),
            pltpu.VMEM((4, 3, 64, 128), BF16),
            pltpu.VMEM((9, 64, 128), BF16),
            pltpu.VMEM((3, 3, 64, 128), BF16),
            pltpu.VMEM((2, n_f, 16, 128), BF16),
            pltpu.VMEM((n_f, 256, 128), BF16),
            pltpu.VMEM((n_f, 256, 128), BF16),
            pltpu.VMEM((n_f, 256, 128), BF16),
            pltpu.VMEM((n_f, 256, 128), BF16),
            pltpu.VMEM((n_y, 256, 128), BF16),
            pltpu.VMEM((n_z, 256, 128), BF16),
            pltpu.VMEM((256, 128), BF16),
            pltpu.VMEM((n_xy, 1024 // n_xy, 128), BF16),
            pltpu.VMEM((n_xy, 1024 // n_xy, 128), BF16),
            pltpu.VMEM((n_xy, 1024 // n_xy, 128), BF16),
            pltpu.VMEM((n_xy, 1024 // n_xy, 128), BF16),
            pltpu.VMEM((2 * n_z, 1024 // n_xy, 128), BF16),
            pltpu.VMEM((n_xy, 1024 // n_xy, 128), BF16),
            pltpu.SemaphoreType.DMA((4,)),
            pltpu.SemaphoreType.DMA((N_SEMS,)),
            pltpu.SemaphoreType.DMA((N_SEMS,)),
        ],
        compiler_params=pltpu.CompilerParams(
            collective_id=0, has_side_effects=True, vmem_limit_bytes=24 * 1024 * 1024
        ),
        name="block",
    )(*(pltpu.with_memory_space_constraint(v, pltpu.HBM) for v in operands))
    return pl.pallas_call(
        functools.partial(unpack, n_f, scales),
        out_shape=(
            shape((16, 1, n_f, 128), BF16),
            shape((64, 2, 2, 256), BF16),
            shape((27, 64, 64), F32),
            shape((27, 16, 64), F32),
        ),
        in_specs=[vmem] * 4,
        out_specs=(vmem,) * 4,
        compiler_params=pltpu.CompilerParams(vmem_limit_bytes=24 * 1024 * 1024),
        name="unpack",
    )(features, volume_grad, fine, bottom)


def solution(mesh):
    n_s, n_f = mesh.shape["space"], mesh.shape["filt"]
    n_z = 4 if n_s % 8 == 0 else 1
    sizes = (n_s, n_f, n_s // (2 * n_z), n_z)
    placed = (
        P(None, "space", "filt", None),
        P(),
        P(None, "filt", None),
        P("filt", "space", None, None),
    )
    return jax.shard_map(
        functools.partial(local, sizes),
        mesh=mesh,
        in_specs=placed,
        out_specs=(
            P("filt", "space", None, None),
            P(None, "space", "filt", None),
            P(),
            P(None, "filt", None),
        ),
        check_vma=False,
    )
```
